128 devices in a mesh: owner: 128 (over z, y, x, core).
Axes of the slice: x: 4, y: 4, z: 4, core: 2. Of those that a mesh axis runs over, the one named last changes fastest.
Arguments:
- frontier: bfloat16 [2048, 1326], P('owner'), may hold values from 0.019897461 to 1
- policy_table: bfloat16 [2048, 1326], replicated, may hold values from 0.019897461 to 1
- first_counts: int32 [2048], P('owner'), may hold values from 1 to 64
- policy_index: int32 [3, 65536], P(None, 'owner'), may hold values from 0 to 2047
- owner_index: int32 [3, 65536], P(None, 'owner'), may hold values from 0 to 127
- next_counts: int32 [2, 65536], P(None, 'owner'), may hold values from 0 to 64, as said below
- value_in: bfloat16 [1326, 1536], replicated, may hold values from -0.15625 to 0.15625
- value_out: bfloat16 [1536, 1326], replicated, may hold values from -0.15625 to 0.15625
Outputs:
- leaf_values: bfloat16 [3, 65536, 1326], P(None, 'owner')
The draws below stay inside these ranges and needn't reach their ends.
Inputs may be any that keep to these rules, and one draw needn't show every extreme that they name: `next_counts`: 0 marks a belief that is not expanded.
All inputs are finite; a program needn't handle non-finite values.
Results may differ from the reference program's by a relative error of at most 0.0067.
Values may be sent and summed in bfloat16 or wider, within the bound.
No kernel may reach another device: no remote copies, remote signals or barrier semaphores. Data moves between devices by JAX's collectives and lax.ppermute only.
A program may use at most 128 MiB of HBM per device.

```python
import math
import jax
import jax.numpy as jnp
from jax import lax

HANDS = 1326
HIDDEN_UNITS = 1536
POLICY = 2048
LEVELS = 3
MAX_CHILDREN = 64
FRONT_DEV = 16
SLOTS = 512
RECV_DEV = 512
NODE_DEV = 384
FRONTIER = 2048
ALL_SLOTS = 65536
N_OWNER = 128


def owner_table(key):
    owner_key = jax.random.fold_in(key, 101)
    return jax.random.randint(owner_key, (LEVELS, SLOTS * N_OWNER), 0, N_OWNER).astype(jnp.int32)


def draw_owner_index(key, part):
    return owner_table(key)


def draw_next_counts(key, part):
    owners = owner_table(key)[:LEVELS - 1]
    grow_key = jax.random.fold_in(key, 11)
    pick_key = jax.random.fold_in(key, 23)
    rate_key = jax.random.fold_in(key, 37)
    shape_all = (LEVELS - 1, SLOTS * N_OWNER)
    exponent = jax.random.randint(rate_key, (LEVELS - 1, N_OWNER), 0, 5).astype(jnp.int32)
    divisor_table = jnp.left_shift(jnp.full((LEVELS - 1, N_OWNER), 4, jnp.int32), exponent)
    divisor = jnp.take_along_axis(divisor_table, owners, axis=1)
    grown = jax.random.randint(grow_key, shape_all, 1, MAX_CHILDREN + 1).astype(jnp.int32)
    picked = jax.random.randint(pick_key, shape_all, 0, 1 << 20).astype(jnp.int32)
    return jnp.where(picked % divisor == 0, grown, 0).astype(jnp.int32)


def plant(result, own_key, low, largest):
    shape = result.shape
    spot = [jax.random.randint(jax.random.fold_in(own_key, axis), (), 0, shape[axis]) for axis in range(len(shape))]
    result = result.at[tuple(spot)].set(low)
    longest = shape.index(max(shape))
    spot[longest] = (spot[longest] + 1) % shape[longest]
    return result.at[tuple(spot)].set(largest)


def block_scale(rng, extent, pieces, least, high):
    def one(position, parts):
        steps = jax.random.uniform(jax.random.fold_in(jax.random.fold_in(rng, 6), position), (parts,), jnp.float32, least / len(pieces), high / len(pieces))
        return jnp.repeat(jnp.exp(steps), extent[position] // parts).reshape((-1,) + (1,) * (len(extent) - position - 1))

    level = one(*pieces[0])
    for cut in pieces[1:]:
        level = level * one(*cut)
    return level


def scatter_about(own_key, extent, spread, bound, held_as=jnp.bfloat16):
    result = spread * jax.random.normal(own_key, extent, jnp.float32)
    return jnp.clip(result, min=-bound, max=bound).astype(held_as)


def setup_inputs(seed: int = 0) -> dict:
    streams_of = jax.random.split(jax.random.key(seed), 9)
    return {
        "frontier": jnp.clip(jnp.exp(math.log(1.0) - 3.9171631 * jax.random.uniform(streams_of[0], (FRONTIER, HANDS), jnp.float32) ** block_scale(streams_of[0], (FRONTIER, HANDS), ((0, 128),), -0.2, 0.2)), 0.019897461, 1.0).astype(jnp.bfloat16),
        "policy_table": jnp.clip(jnp.exp(jax.random.uniform(streams_of[1], (POLICY, HANDS), jnp.float32, math.log(0.019897461), math.log(1.0))), 0.019897461, 1.0).astype(jnp.bfloat16),
        "first_counts": plant(jax.random.randint(streams_of[2], (FRONTIER,), 1, MAX_CHILDREN + 1), jax.random.fold_in(streams_of[2], 1), 1, MAX_CHILDREN).astype(jnp.int32),
        "policy_index": plant(jax.random.randint(streams_of[3], (LEVELS, ALL_SLOTS), 0, POLICY), jax.random.fold_in(streams_of[3], 1), 0, POLICY - 1).astype(jnp.int32),
        "owner_index": draw_owner_index(jax.random.fold_in(streams_of[8], 71), 0),
        "next_counts": draw_next_counts(jax.random.fold_in(streams_of[8], 71), 0),
        "value_in": scatter_about(streams_of[6], (HANDS, HIDDEN_UNITS), HANDS ** -0.5, 0.15625),
        "value_out": scatter_about(streams_of[7], (HIDDEN_UNITS, HANDS), HIDDEN_UNITS ** -0.5, 0.15625),
    }


def count_slots(counts, slots):
    count_ends = jnp.cumsum(counts).astype(jnp.int32)
    child_total = jnp.minimum(count_ends[-1], slots).astype(jnp.int32)
    slot_index = jnp.arange(slots, dtype=jnp.int32)
    segment = jnp.sum((count_ends[None, :] <= slot_index[:, None]).astype(jnp.int32), axis=1).astype(jnp.int32)
    segment = jnp.minimum(segment, counts.shape[0] - 1).astype(jnp.int32)
    return child_total, slot_index, segment


def form_children(parent_rows, policy_rows, kept_mask):
    children = parent_rows.astype(jnp.float32) * policy_rows.astype(jnp.float32)
    child_mass = jnp.sum(children, axis=1)
    child_mass = jnp.where(kept_mask, child_mass, jnp.float32(1.0))
    rescale = children.shape[1] / child_mass
    return jnp.where(kept_mask[:, None], children * rescale[:, None], jnp.float32(0.0)).astype(jnp.bfloat16)


def bucket_sources(owners, kept_mask, devices, capacity):
    slot_count = owners.shape[0]
    onehot = ((owners[:, None] == jnp.arange(devices, dtype=jnp.int32)[None, :]) & kept_mask[:, None]).astype(jnp.int32)
    rank_owner = (jnp.sum(jnp.cumsum(onehot, axis=0).astype(jnp.int32) * onehot, axis=1) - 1).astype(jnp.int32)
    sent_mask = kept_mask & (rank_owner < capacity)
    destination = jnp.where(sent_mask, owners * capacity + rank_owner, devices * capacity).astype(jnp.int32)
    source = jnp.full((devices * capacity + 1,), slot_count, jnp.int32)
    source = source.at[destination].set(jnp.arange(slot_count, dtype=jnp.int32))
    return source[: devices * capacity]


def value_net(ranges, value_in, value_out):
    hidden = jnp.maximum(jnp.dot(ranges, value_in, preferred_element_type=jnp.float32), jnp.float32(0.0)).astype(jnp.bfloat16)
    return jnp.dot(hidden, value_out, preferred_element_type=jnp.float32).astype(jnp.bfloat16)


def reference(frontier, policy_table, first_counts, policy_index, owner_index, next_counts, value_in, value_out):
    devices = N_OWNER
    capacity = RECV_DEV // devices
    kept_limit = NODE_DEV * devices
    parents = frontier.reshape(devices, FRONT_DEV, HANDS)
    counts = first_counts.reshape(devices, FRONT_DEV)
    level_values = []
    for depth in range(LEVELS):
        policy_rows = policy_index[depth].reshape(devices, SLOTS)
        owner_rows = owner_index[depth].reshape(devices, SLOTS)
        if depth < LEVELS - 1:
            next_rows = next_counts[depth].reshape(devices, SLOTS)
        else:
            next_rows = jnp.zeros((devices, SLOTS), jnp.int32)
        totals = jax.vmap(lambda row: count_slots(row, SLOTS)[0])(counts).astype(jnp.int32)
        offsets = (jnp.cumsum(totals) - totals).astype(jnp.int32)

        def device_step(items):
            parent_block, count_block, policy_block, owner_block, next_block, offset = items
            child_total, slot_index, segment = count_slots(count_block, SLOTS)
            kept_mask = (slot_index < child_total) & (offset + slot_index < kept_limit)
            children = form_children(parent_block[segment], policy_table[policy_block], kept_mask)
            source = bucket_sources(owner_block, kept_mask, devices, capacity)
            padded_rows = jnp.concatenate([children, jnp.zeros((1, HANDS), jnp.bfloat16)], axis=0)
            padded_next = jnp.concatenate([next_block, jnp.zeros((1,), jnp.int32)])
            return padded_rows[source], padded_next[source]

        outgoing, outgoing_counts = lax.map(device_step, (parents, counts, policy_rows, owner_rows, next_rows, offsets))
        parents = outgoing.reshape(devices, devices, capacity, HANDS).transpose(1, 0, 2, 3).reshape(devices, devices * capacity, HANDS)
        counts = outgoing_counts.reshape(devices, devices, capacity).transpose(1, 0, 2).reshape(devices, devices * capacity)
        values = lax.map(lambda block: value_net(block, value_in, value_out), parents)
        level_values.append(values.reshape(devices * devices * capacity, HANDS))
    return jnp.stack(level_values)
```

```python
import jax
import jax.numpy as jnp
from jax import lax
from jax.experimental import pallas as pl
from jax.experimental.pallas import tpu as pltpu
from jax.sharding import Mesh
from jax.sharding import PartitionSpec as P

HANDS = 1326
HIDDEN = 1536
POLICY = 2048
SLOTS = 512
DEVICES = 128
CHIPS = 64
FRONT = 16
CAP = 4
KEPT = 384 * DEVICES
CHUNKS = 11
WIDTH = CHUNKS * 128
FROWS = FRONT * CHUNKS
COMMON = 38
TROWS = COMMON + 2
BROWS = FROWS + TROWS
STRIDE = 16
BLOCK = 256
OWNER = ("owner_0", "owner_1", "owner_2", "owner_3")
F32 = jnp.float32
BF16 = jnp.bfloat16
I32 = jnp.int32


def iota(shape, dim):
    return lax.broadcasted_iota(I32, shape, dim)


def mm(a, b, dims):
    return lax.dot_general(a.astype(BF16), b.astype(BF16), (dims, ((), ())), preferred_element_type=F32)


NN = ((1,), (0,))
NT = ((1,), (1,))
TN = ((0,), (0,))


def tables_kernel(first_ref, owner_ref, policy_ref, next_ref, common_ref, spec_ref):
    lane = iota((1, SLOTS), 1)
    segment = jnp.zeros((1, SLOTS), I32)
    running = jnp.int32(0)
    for k in range(FRONT):
        running = running + first_ref[k]
        if k < FRONT - 1:
            segment = segment + (running <= lane).astype(I32)
    total = jnp.minimum(running, SLOTS)
    upper = (iota((SLOTS, SLOTS), 0) <= iota((SLOTS, SLOTS), 1)).astype(F32).astype(BF16)
    rows = []
    for level in range(3):
        hit = iota((DEVICES, SLOTS), 0) == owner_ref[level : level + 1, :]
        rank = mm(hit.astype(F32), upper, NN)
        policy = policy_ref[level : level + 1, :]
        fields = [lane - SLOTS // 2, jnp.ones_like(lane), lax.shift_right_logical(policy, 4), policy & 15]
        fields.append(next_ref[level : level + 1, :] if level < 2 else jnp.zeros_like(lane))
        fields.append(segment)
        values = jnp.concatenate(fields + [jnp.zeros_like(lane)] * 2, axis=0).astype(F32)
        found = []
        for r in range(CAP):
            mask = jnp.where(hit & (rank == r + 1), 1.0, 0.0)
            found.append(mm(values, mask, NT))
        slot = [f[0:1] + (SLOTS // 2) * (1.0 - f[1:2]) for f in found]
        high = [f[2:3] for f in found]
        low = [f[3:4] for f in found]
        count = [f[4:5] for f in found]
        parent = [f[5:6] for f in found]
        if level == 0:
            rows += slot + count + high + low + parent
        elif level == 1:
            rows += slot + count + high + low
        else:
            last = slot + high + low
    lanes = jnp.zeros((1, DEVICES), F32)
    zero = [lanes]
    common = rows + [lanes + (total - SLOTS // 2).astype(F32)] + zero
    common = jnp.concatenate(common + zero * (40 - len(common)), axis=0)
    common_ref[...] = common.astype(BF16)
    spec = jnp.concatenate(rows + last + zero * (DEVICES - len(rows) - len(last)), axis=0)
    spec_ref[...] = jnp.transpose(spec).astype(BF16)


def tables(first, owner, policy, following):
    vm = pl.BlockSpec(memory_space=pltpu.VMEM)
    return pl.pallas_call(
        tables_kernel,
        out_shape=[
            jax.ShapeDtypeStruct((40, DEVICES), BF16),
            jax.ShapeDtypeStruct((DEVICES, DEVICES), BF16),
        ],
        in_specs=[pl.BlockSpec(memory_space=pltpu.SMEM), vm, vm, vm],
        out_specs=[vm, vm],
        name="tables",
    )(first, owner, policy, following)


def paths_kernel(core_ref, mine_ref, other_ref, out_ref, wide_ref):
    core = core_ref[0]
    for h, ref in enumerate((mine_ref, other_ref)):
        wide_ref[h] = ref[...].astype(F32)

    def field(h, row):
        return wide_ref[h, pl.ds(row, CHIPS, stride=TROWS), :]

    def full(base):
        return jnp.concatenate([field(h, base + r) for r in range(CAP) for h in range(2)], axis=0)

    n = 2 * CAP * CHIPS

    def places(shape, dim):
        i = iota(shape, dim)
        g, h, r = i & 63, lax.shift_right_logical(i, 6) & 1, lax.shift_right_logical(i, 7)
        return g, h, r, 2 * g + (h ^ core)

    def flag(x):
        return jnp.where(x, 1.0, 0.0).astype(BF16)

    half = SLOTS // 2
    g, h, r, s_row = places((n, DEVICES), 0)
    location = (h * CHIPS + g).astype(F32)
    s_f = s_row.astype(F32)
    s_loc_lane = 2 * (iota((n, DEVICES), 1) & 63) + (lax.shift_right_logical(iota((n, DEVICES), 1), 6) ^ core)
    lane = iota((n, DEVICES), 1)
    _, _, ra, sa = places((n, n), 0)
    _, _, rb, sb = places((n, n), 1)
    before = flag(sb * CAP + rb <= sa * CAP + ra)
    loc0 = iota((DEVICES, DEVICES), 0)
    s0 = 2 * (loc0 & 63) + (lax.shift_right_logical(loc0, 6) ^ core)
    d1 = iota((DEVICES, DEVICES), 1)
    turn = flag(s0 == d1)
    d_lane = iota((1, DEVICES), 1)
    d_f = d_lane.astype(F32)
    d_location = ((d_lane & 1) ^ core) * CHIPS + lax.shift_right_logical(d_lane, 1)

    spec = jnp.concatenate(
        [jnp.where(core == 0, field(k, COMMON), field(k, COMMON + 1)) for k in range(2)], axis=0
    )
    own = mm(spec, turn, TN)

    def mine(base):
        return own[base : base + CAP]

    totals = jnp.concatenate([field(0, 36), field(1, 36)], axis=0)
    offset = mm(flag(s_loc_lane < s_row), totals, NN) + half * s_f
    total = mm(flag(s_loc_lane == s_row), totals, NN) + half
    slot = full(0) + half
    kept = (slot < total) & (offset + slot < KEPT)
    count2 = jnp.where(kept, full(4), 0.0)
    cum2 = mm(before, count2, NN)
    ex2 = cum2 - count2
    total2 = jnp.minimum(jnp.sum(count2, axis=0, keepdims=True), float(SLOTS))
    total1_d = mm(totals, turn, TN)[0:1] + half
    offset1_d = mm(totals, flag(s0 < d1), TN)[0:1] + half * d_f
    j1 = mine(0) + half
    ok1 = (j1 < total1_d) & (offset1_d + j1 < KEPT)
    floc1 = d_location.astype(F32) * FRONT + mine(16)
    q1 = mine(8) * 16 + mine(12)
    wide2 = jnp.broadcast_to(total2 - half, (DEVICES, DEVICES))
    below = flag(loc0 < d1)
    less = flag(lane < s_row)
    same = flag(lane == s_row)
    offset = mm(less, wide2, NT) + half * s_f
    total = mm(same, wide2, NT) + half
    slot2 = full(20) + half
    kept = (slot2 < total) & (offset + slot2 < KEPT)
    count3 = jnp.where(kept, full(24), 0.0)
    cum3 = mm(before, count3, NN)
    ex3 = cum3 - count3
    total3 = jnp.minimum(jnp.sum(count3, axis=0, keepdims=True), float(SLOTS))
    j2 = mine(20) + half
    offset2_d = mm(wide2, below, NN)[0:1] + half * d_f
    ok2 = (j2 < total2) & (offset2_d + j2 < KEPT)
    parent1 = full(16)
    high1, low1 = full(8), full(12)
    path1 = (location * FRONT + parent1) * POLICY + high1 * 16 + low1
    path2 = []
    for r in range(CAP):
        j = j2[r : r + 1]
        path2.append(jnp.sum(jnp.where((ex2 <= j) & (j < cum2), path1, 0.0), axis=0, keepdims=True))
    path2 = jnp.concatenate(path2, axis=0).astype(I32)
    wide3 = jnp.broadcast_to(total3 - half, (DEVICES, DEVICES))
    offset3_d = mm(wide3, below, NN)[0:1] + half * d_f
    j3 = mine(36) + half
    ok3 = (j3 < total3) & (offset3_d + j3 < KEPT)
    policy2 = full(28) * 16 + full(32)
    via = s_f * 1024 + slot2
    stack = jnp.concatenate(
        [
            (jnp.minimum(cum2, float(SLOTS)) - half).astype(BF16),
            (jnp.minimum(ex2, float(SLOTS)) - half).astype(BF16),
            parent1.astype(BF16),
            high1.astype(BF16),
            low1.astype(BF16),
        ],
        axis=0,
    )
    path3, policy3 = [], []
    for r in range(CAP):
        j = j3[r : r + 1]
        hit = (ex3 <= j) & (j < cum3)
        policy3.append(jnp.sum(jnp.where(hit, policy2, 0.0), axis=0, keepdims=True))
        through = jnp.sum(jnp.where(hit, via, 0.0), axis=0, keepdims=True).astype(I32)
        device = lax.shift_right_logical(through, 10)
        jj = (through & 1023).astype(F32) - half
        got = mm(stack, flag(loc0 == device), NN)
        hit = (got[n : 2 * n] <= jj) & (jj < got[:n])
        path = (location * FRONT + got[2 * n : 3 * n]) * POLICY + got[3 * n : 4 * n] * 16 + got[4 * n :]
        path3.append(jnp.sum(jnp.where(hit, path, 0.0), axis=0, keepdims=True))
    path3 = jnp.concatenate(path3, axis=0).astype(I32)
    policy3 = jnp.concatenate(policy3, axis=0).astype(I32)

    def last(ok, base):
        return jnp.where(ok, (mine(base) * 16 + mine(base + 4)).astype(I32), POLICY)

    out_ref[0:4] = floc1.astype(I32)
    out_ref[4:8] = jnp.where(ok1, q1.astype(I32), POLICY)
    out_ref[8:12] = lax.shift_right_logical(path2, 11)
    out_ref[12:16] = path2 & (POLICY - 1)
    out_ref[16:20] = last(ok2, 28)
    out_ref[20:24] = lax.shift_right_logical(path3, 11)
    out_ref[24:28] = path3 & (POLICY - 1)
    out_ref[28:32] = policy3
    out_ref[32:36] = last(ok3, 40)
    out_ref[36:40] = jnp.zeros((4, DEVICES), I32)


def paths(core, mine, other):
    vm = pl.BlockSpec(memory_space=pltpu.VMEM)
    return pl.pallas_call(
        paths_kernel,
        out_shape=jax.ShapeDtypeStruct((40, DEVICES), I32),
        in_specs=[pl.BlockSpec(memory_space=pltpu.SMEM), vm, vm],
        out_specs=vm,
        scratch_shapes=[pltpu.VMEM((2, CHIPS * TROWS, 128), F32)],
        name="paths",
    )(core, mine, other)


FIELDS = ((0, (4,)), (8, (12, 16)), (20, (24, 28, 32)))


def values_kernel(
    paths_ref, mine_ref, other_ref, policy_ref, in_ref, out_w_ref, out_ref, front_ref, a_ref, b_ref, c_ref, x_ref, h_ref
):
    for half, ref in enumerate((mine_ref, other_ref)):

        @pl.loop(0, CHIPS)
        def _(i, half=half, ref=ref):
            at = pl.multiple_of((half * CHIPS + i) * FROWS, FROWS)
            front_ref[pl.ds(at, FROWS), :] = ref[i, :FROWS, :].astype(F32)

    def rows_of(table, index):
        at = index * CHUNKS
        return table[pl.ds(at, 8), :], table[pl.ds(at + 8, 8), :]

    def chunk(ref, start, k):
        return ref[pl.ds(start * STRIDE + k, 8, stride=STRIDE), :]

    for level in range(3):
        place, policies = FIELDS[level]
        hold = (a_ref, b_ref, c_ref)[: level + 1]
        for block in range(SLOTS // BLOCK):

            @pl.loop(0, BLOCK // 8)
            def _(i, block=block, place=place, policies=policies, hold=hold):
                for e in range(8):
                    s = block * (BLOCK // CAP) + i * 2 + e // CAP
                    r = e % CAP
                    at = pl.multiple_of((i * 8 + e) * STRIDE, STRIDE)
                    for k, (base, ref) in enumerate(zip(policies, hold)):
                        lo, hi = rows_of(policy_ref, paths_ref[base + r, s])
                        if k == 0:
                            flo, fhi = rows_of(front_ref, paths_ref[place + r, s])
                            lo, hi = lo * flo, hi * fhi
                        ref[pl.ds(at, 8), :] = lo
                        ref[pl.ds(pl.multiple_of(at + 8, 8), 8), :] = hi

            @pl.loop(0, BLOCK // 16)
            def _(i, block=block, hold=hold):
                child = [[None] * CHUNKS, [None] * CHUNKS]
                for u in range(2):
                    start = i * 16 + u * 8
                    for step, ref in enumerate(hold):
                        terms = [chunk(ref, start, k) for k in range(CHUNKS)]
                        if step:
                            terms = [t * c for t, c in zip(terms, child[u])]
                        mass = terms[0]
                        for t in terms[1:]:
                            mass = mass + t
                        mass = jnp.sum(mass, axis=1, keepdims=True)
                        scale = jnp.where(mass > 0, HANDS / mass, 0.0)
                        child[u] = [(t * scale).astype(BF16).astype(F32) for t in terms]
                at = pl.multiple_of(block * BLOCK + i * 16, 16)
                for k in range(CHUNKS):
                    both = jnp.concatenate([child[0][k], child[1][k]], axis=0).astype(BF16)
                    x_ref[pl.ds(at, 16), k * 128 : (k + 1) * 128] = both

        for block in range(2):
            rows = slice(block * 256, block * 256 + 256)
            for cut in range(0, HIDDEN, 512):
                hidden = jnp.dot(x_ref[rows, :], in_ref[:, cut : cut + 512], preferred_element_type=F32)
                h_ref[rows, cut : cut + 512] = jnp.maximum(hidden, 0.0).astype(BF16)
        for cut in range(0, HANDS, 256):
            end = min(cut + 256, HANDS)
            value = lax.dot_general(out_w_ref[cut:end, :], h_ref[...], (NT, ((), ())), preferred_element_type=F32)
            out_ref[level, cut:end, :] = value.astype(BF16)


def values(paths, mine, other, policy, value_in, value_out):
    vm = pl.BlockSpec(memory_space=pltpu.VMEM)
    hold = pltpu.VMEM((BLOCK * STRIDE, 128), F32)
    return pl.pallas_call(
        values_kernel,
        out_shape=jax.ShapeDtypeStruct((3, HANDS, SLOTS), BF16),
        in_specs=[pl.BlockSpec(memory_space=pltpu.SMEM), vm, vm, vm, vm, vm],
        out_specs=vm,
        scratch_shapes=[
            pltpu.VMEM((DEVICES * FROWS + 8, 128), F32),
            hold,
            hold,
            hold,
            pltpu.VMEM((SLOTS, WIDTH), BF16),
            pltpu.VMEM((SLOTS, HIDDEN), BF16),
        ],
        compiler_params=pltpu.CompilerParams(vmem_limit_bytes=62 * 1024 * 1024),
        name="values",
    )(paths, mine, other, policy, value_in, value_out)


def on_device(frontier, policy_table, first, policy_index, owner_index, following, value_in, value_out):
    core = lax.axis_index("owner_3").astype(I32)[None]
    common, spec = tables(first, owner_index, policy_index, following)
    ranges = jnp.pad(frontier, ((0, 0), (0, WIDTH - HANDS))).reshape(FROWS, 128)
    shared = jnp.concatenate([ranges, common[:COMMON]], axis=0)
    block = jnp.concatenate(
        [jnp.broadcast_to(shared[None], (CHIPS,) + shared.shape), spec.reshape(CHIPS, 2, 128)], axis=1
    )
    mine = lax.all_to_all(block, OWNER[:3], split_axis=0, concat_axis=0, tiled=True)
    other = lax.ppermute(mine, OWNER[3], [(0, 1), (1, 0)])
    policy = jnp.pad(policy_table, ((0, 1), (0, WIDTH - HANDS))).astype(F32).reshape((POLICY + 1) * CHUNKS, 128)
    policy = jnp.pad(policy, ((0, 13), (0, 0)))
    weights_in = jnp.pad(value_in, ((0, WIDTH - HANDS), (0, 0)))

    def part(x):
        return x[:, FROWS:, :].reshape(CHIPS * TROWS, 128)

    found = paths(core, part(mine), part(other))
    out = values(found, mine, other, policy, weights_in, jnp.transpose(value_out))
    return jnp.transpose(out, (0, 2, 1))


def solution(mesh):
    torus = Mesh(mesh.devices.reshape(4, 4, 4, 2), OWNER)
    placed = (P(OWNER, None), P(), P(OWNER), P(None, OWNER), P(None, OWNER), P(None, OWNER), P(), P())
    return jax.shard_map(on_device, mesh=torus, in_specs=placed, out_specs=P(None, OWNER, None), check_vma=False)
```

```python
import jax
import jax.numpy as jnp
from jax import lax
from jax.experimental import pallas as pl
from jax.experimental.pallas import tpu as pltpu
from jax.sharding import Mesh
from jax.sharding import PartitionSpec as P

HANDS = 1326
HIDDEN = 1536
POLICY = 2048
SLOTS = 512
DEVICES = 128
CHIPS = 64
FRONT = 16
CAP = 4
KEPT = 384 * DEVICES
CHUNKS = 11
WIDTH = CHUNKS * 128
FROWS = FRONT * CHUNKS
COMMON = 38
TROWS = COMMON + 2
BROWS = FROWS + TROWS
STRIDE = 17
BLOCK = 256
UNROLL = 64
OWNER = ("owner_0", "owner_1", "owner_2", "owner_3")
F32 = jnp.float32
BF16 = jnp.bfloat16
I32 = jnp.int32


def iota(shape, dim):
    return lax.broadcasted_iota(I32, shape, dim)


def mm(a, b, dims):
    return lax.dot_general(a.astype(BF16), b.astype(BF16), (dims, ((), ())), preferred_element_type=F32)


NN = ((1,), (0,))
NT = ((1,), (1,))
TN = ((0,), (0,))


def tables_kernel(first_ref, owner_ref, policy_ref, next_ref, common_ref, spec_ref):
    lane = iota((1, SLOTS), 1)
    segment = jnp.zeros((1, SLOTS), I32)
    running = jnp.int32(0)
    for k in range(FRONT):
        running = running + first_ref[k]
        if k < FRONT - 1:
            segment = segment + (running <= lane).astype(I32)
    total = jnp.minimum(running, SLOTS)
    upper = (iota((SLOTS, SLOTS), 0) <= iota((SLOTS, SLOTS), 1)).astype(F32).astype(BF16)
    rows = []
    for level in range(3):
        hit = iota((DEVICES, SLOTS), 0) == owner_ref[level : level + 1, :]
        rank = mm(hit.astype(F32), upper, NN)
        policy = policy_ref[level : level + 1, :]
        fields = [lane - SLOTS // 2, jnp.ones_like(lane), lax.shift_right_logical(policy, 4), policy & 15]
        fields.append(next_ref[level : level + 1, :] if level < 2 else jnp.zeros_like(lane))
        fields.append(segment)
        values = jnp.concatenate(fields + [jnp.zeros_like(lane)] * 2, axis=0).astype(F32)
        found = []
        for r in range(CAP):
            mask = jnp.where(hit & (rank == r + 1), 1.0, 0.0)
            found.append(mm(values, mask, NT))
        slot = [f[0:1] + (SLOTS // 2) * (1.0 - f[1:2]) for f in found]
        high = [f[2:3] for f in found]
        low = [f[3:4] for f in found]
        count = [f[4:5] for f in found]
        parent = [f[5:6] for f in found]
        if level == 0:
            rows += slot + count + high + low + parent
        elif level == 1:
            rows += slot + count + high + low
        else:
            last = slot + high + low
    lanes = jnp.zeros((1, DEVICES), F32)
    zero = [lanes]
    common = rows + [lanes + (total - SLOTS // 2).astype(F32)] + zero
    common = jnp.concatenate(common + zero * (40 - len(common)), axis=0)
    common_ref[...] = common.astype(BF16)
    spec = jnp.concatenate(rows + last + zero * (DEVICES - len(rows) - len(last)), axis=0)
    spec_ref[...] = jnp.transpose(spec).astype(BF16)


def tables(first, owner, policy, following):
    vm = pl.BlockSpec(memory_space=pltpu.VMEM)
    return pl.pallas_call(
        tables_kernel,
        out_shape=[
            jax.ShapeDtypeStruct((40, DEVICES), BF16),
            jax.ShapeDtypeStruct((DEVICES, DEVICES), BF16),
        ],
        in_specs=[pl.BlockSpec(memory_space=pltpu.SMEM), vm, vm, vm],
        out_specs=[vm, vm],
        name="tables",
    )(first, owner, policy, following)


def paths_kernel(core_ref, mine_ref, other_ref, out_ref, wide_ref):
    core = core_ref[0]
    for h, ref in enumerate((mine_ref, other_ref)):
        wide_ref[h] = ref[...].astype(F32)

    def field(h, row):
        return wide_ref[h, pl.ds(row, CHIPS, stride=TROWS), :]

    def full(base):
        return jnp.concatenate([field(h, base + r) for r in range(CAP) for h in range(2)], axis=0)

    n = 2 * CAP * CHIPS

    def places(shape, dim):
        i = iota(shape, dim)
        g, h, r = i & 63, lax.shift_right_logical(i, 6) & 1, lax.shift_right_logical(i, 7)
        return g, h, r, 2 * g + (h ^ core)

    def flag(x):
        return jnp.where(x, 1.0, 0.0).astype(BF16)

    half = SLOTS // 2
    g, h, r, s_row = places((n, DEVICES), 0)
    location = (h * CHIPS + g).astype(F32)
    s_f = s_row.astype(F32)
    s_loc_lane = 2 * (iota((n, DEVICES), 1) & 63) + (lax.shift_right_logical(iota((n, DEVICES), 1), 6) ^ core)
    lane = iota((n, DEVICES), 1)
    _, _, ra, sa = places((n, n), 0)
    _, _, rb, sb = places((n, n), 1)
    before = flag(sb * CAP + rb <= sa * CAP + ra)
    loc0 = iota((DEVICES, DEVICES), 0)
    s0 = 2 * (loc0 & 63) + (lax.shift_right_logical(loc0, 6) ^ core)
    d1 = iota((DEVICES, DEVICES), 1)
    turn = flag(s0 == d1)
    d_lane = iota((1, DEVICES), 1)
    d_f = d_lane.astype(F32)
    d_location = ((d_lane & 1) ^ core) * CHIPS + lax.shift_right_logical(d_lane, 1)

    spec = jnp.concatenate(
        [jnp.where(core == 0, field(k, COMMON), field(k, COMMON + 1)) for k in range(2)], axis=0
    )
    own = mm(spec, turn, TN)

    def mine(base):
        return own[base : base + CAP]

    totals = jnp.concatenate([field(0, 36), field(1, 36)], axis=0)
    offset = mm(flag(s_loc_lane < s_row), totals, NN) + half * s_f
    total = mm(flag(s_loc_lane == s_row), totals, NN) + half
    slot = full(0) + half
    kept = (slot < total) & (offset + slot < KEPT)
    count2 = jnp.where(kept, full(4), 0.0)
    cum2 = mm(before, count2, NN)
    ex2 = cum2 - count2
    total2 = jnp.minimum(jnp.sum(count2, axis=0, keepdims=True), float(SLOTS))
    total1_d = mm(totals, turn, TN)[0:1] + half
    offset1_d = mm(totals, flag(s0 < d1), TN)[0:1] + half * d_f
    j1 = mine(0) + half
    ok1 = (j1 < total1_d) & (offset1_d + j1 < KEPT)
    floc1 = d_location.astype(F32) * FRONT + mine(16)
    q1 = mine(8) * 16 + mine(12)
    wide2 = jnp.broadcast_to(total2 - half, (DEVICES, DEVICES))
    below = flag(loc0 < d1)
    less = flag(lane < s_row)
    same = flag(lane == s_row)
    offset = mm(less, wide2, NT) + half * s_f
    total = mm(same, wide2, NT) + half
    slot2 = full(20) + half
    kept = (slot2 < total) & (offset + slot2 < KEPT)
    count3 = jnp.where(kept, full(24), 0.0)
    cum3 = mm(before, count3, NN)
    ex3 = cum3 - count3
    total3 = jnp.minimum(jnp.sum(count3, axis=0, keepdims=True), float(SLOTS))
    j2 = mine(20) + half
    offset2_d = mm(wide2, below, NN)[0:1] + half * d_f
    ok2 = (j2 < total2) & (offset2_d + j2 < KEPT)
    parent1 = full(16)
    high1, low1 = full(8), full(12)
    path1 = (location * FRONT + parent1) * POLICY + high1 * 16 + low1
    path2 = []
    for r in range(CAP):
        j = j2[r : r + 1]
        path2.append(jnp.sum(jnp.where((ex2 <= j) & (j < cum2), path1, 0.0), axis=0, keepdims=True))
    path2 = jnp.concatenate(path2, axis=0).astype(I32)
    wide3 = jnp.broadcast_to(total3 - half, (DEVICES, DEVICES))
    offset3_d = mm(wide3, below, NN)[0:1] + half * d_f
    j3 = mine(36) + half
    ok3 = (j3 < total3) & (offset3_d + j3 < KEPT)
    policy2 = full(28) * 16 + full(32)
    via = s_f * 1024 + slot2
    stack = jnp.concatenate(
        [
            (jnp.minimum(cum2, float(SLOTS)) - half).astype(BF16),
            (jnp.minimum(ex2, float(SLOTS)) - half).astype(BF16),
            parent1.astype(BF16),
            high1.astype(BF16),
            low1.astype(BF16),
        ],
        axis=0,
    )
    path3, policy3 = [], []
    for r in range(CAP):
        j = j3[r : r + 1]
        hit = (ex3 <= j) & (j < cum3)
        policy3.append(jnp.sum(jnp.where(hit, policy2, 0.0), axis=0, keepdims=True))
        through = jnp.sum(jnp.where(hit, via, 0.0), axis=0, keepdims=True).astype(I32)
        device = lax.shift_right_logical(through, 10)
        jj = (through & 1023).astype(F32) - half
        got = mm(stack, flag(loc0 == device), NN)
        hit = (got[n : 2 * n] <= jj) & (jj < got[:n])
        path = (location * FRONT + got[2 * n : 3 * n]) * POLICY + got[3 * n : 4 * n] * 16 + got[4 * n :]
        path3.append(jnp.sum(jnp.where(hit, path, 0.0), axis=0, keepdims=True))
    path3 = jnp.concatenate(path3, axis=0).astype(I32)
    policy3 = jnp.concatenate(policy3, axis=0).astype(I32)

    def last(ok, base):
        return jnp.where(ok, (mine(base) * 16 + mine(base + 4)).astype(I32), POLICY)

    out_ref[0:4] = floc1.astype(I32)
    out_ref[4:8] = jnp.where(ok1, q1.astype(I32), POLICY)
    out_ref[8:12] = lax.shift_right_logical(path2, 11)
    out_ref[12:16] = path2 & (POLICY - 1)
    out_ref[16:20] = last(ok2, 28)
    out_ref[20:24] = lax.shift_right_logical(path3, 11)
    out_ref[24:28] = path3 & (POLICY - 1)
    out_ref[28:32] = policy3
    out_ref[32:36] = last(ok3, 40)
    out_ref[36:40] = jnp.zeros((4, DEVICES), I32)


def paths(core, mine, other):
    vm = pl.BlockSpec(memory_space=pltpu.VMEM)
    return pl.pallas_call(
        paths_kernel,
        out_shape=jax.ShapeDtypeStruct((40, DEVICES), I32),
        in_specs=[pl.BlockSpec(memory_space=pltpu.SMEM), vm, vm],
        out_specs=vm,
        scratch_shapes=[pltpu.VMEM((2, CHIPS * TROWS, 128), F32)],
        name="paths",
    )(core, mine, other)


FIELDS = ((0, (4,)), (8, (12, 16)), (20, (24, 28, 32)))


def values_kernel(
    paths_ref, mine_ref, other_ref, policy_ref, in_ref, out_w_ref, out_ref, front_ref, a_ref, b_ref, c_ref, y_ref, x_ref, h_ref
):
    for half, ref in enumerate((mine_ref, other_ref)):

        @pl.loop(0, CHIPS)
        def _(i, half=half, ref=ref):
            at = pl.multiple_of((half * CHIPS + i) * FROWS, FROWS)
            front_ref[pl.ds(at, FROWS), :] = ref[i, :FROWS, :].astype(F32)

    def rows_of(table, index):
        at = index * CHUNKS
        return table[pl.ds(at, 8), :], table[pl.ds(at + 8, 8), :]

    def rounded(t):
        return t.astype(BF16).astype(F32)

    def chunk(ref, start, k):
        return ref[pl.ds(start * STRIDE + k, 8, stride=STRIDE), :]

    for level in range(3):
        place, policies = FIELDS[level]
        hold = (a_ref, b_ref, c_ref)[: level + 1]
        for block in range(SLOTS // BLOCK):

            @pl.loop(0, BLOCK // 8)
            def _(i, block=block, place=place, policies=policies, hold=hold):
                for e in range(8):
                    s = block * (BLOCK // CAP) + i * 2 + e // CAP
                    r = e % CAP
                    at = (i * 8 + e) * STRIDE
                    for k, (base, ref) in enumerate(zip(policies, hold)):
                        lo, hi = rows_of(policy_ref, paths_ref[base + r, s])
                        if k == 0:
                            flo, fhi = rows_of(front_ref, paths_ref[place + r, s])
                            lo, hi = lo * flo, hi * fhi
                        ref[pl.ds(at, 8), :] = lo
                        ref[pl.ds(at + 8, 8), :] = hi

            @pl.loop(0, BLOCK // UNROLL)
            def _(i, block=block, hold=hold):
                scales = [None] * (UNROLL // 8)
                for step, ref in enumerate(hold):
                    masses = []
                    for u in range(UNROLL // 8):
                        start = i * UNROLL + u * 8
                        at = pl.ds(pl.multiple_of(start, 8), 8)
                        mass = None
                        for k in range(CHUNKS):
                            term = chunk(ref, start, k)
                            cut = slice(k * 128, (k + 1) * 128)
                            if step:
                                term = term * rounded(y_ref[at, cut] * scales[u])
                            y_ref[at, cut] = term
                            mass = term if mass is None else mass + term
                        masses.append(mass)
                    masses = [jnp.sum(m, axis=1, keepdims=True) for m in masses]
                    scales = [jnp.where(m > 0, HANDS / m, 0.0) for m in masses]
                for u in range(UNROLL // 16):
                    start = i * UNROLL + u * 16
                    at = pl.multiple_of(block * BLOCK + start, 16)
                    for k in range(CHUNKS):
                        cut = slice(k * 128, (k + 1) * 128)
                        pair = [
                            y_ref[pl.ds(pl.multiple_of(start + v * 8, 8), 8), cut] * scales[2 * u + v] for v in range(2)
                        ]
                        x_ref[pl.ds(at, 16), cut] = jnp.concatenate(pair, axis=0).astype(BF16)

        for block in range(2):
            rows = slice(block * 256, block * 256 + 256)
            for cut in range(0, HIDDEN, 512):
                hidden = jnp.dot(x_ref[rows, :], in_ref[:, cut : cut + 512], preferred_element_type=F32)
                h_ref[rows, cut : cut + 512] = jnp.maximum(hidden, 0.0).astype(BF16)
        for cut in range(0, HANDS, 256):
            end = min(cut + 256, HANDS)
            value = lax.dot_general(out_w_ref[cut:end, :], h_ref[...], (NT, ((), ())), preferred_element_type=F32)
            out_ref[level, cut:end, :] = value.astype(BF16)


def values(paths, mine, other, policy, value_in, value_out):
    vm = pl.BlockSpec(memory_space=pltpu.VMEM)
    hold = pltpu.VMEM((BLOCK * STRIDE + 16, 128), F32)
    return pl.pallas_call(
        values_kernel,
        out_shape=jax.ShapeDtypeStruct((3, HANDS, SLOTS), BF16),
        in_specs=[pl.BlockSpec(memory_space=pltpu.SMEM), vm, vm, vm, vm, vm],
        out_specs=vm,
        scratch_shapes=[
            pltpu.VMEM((DEVICES * FROWS + 8, 128), F32),
            hold,
            hold,
            hold,
            pltpu.VMEM((BLOCK, WIDTH), F32),
            pltpu.VMEM((SLOTS, WIDTH), BF16),
            pltpu.VMEM((SLOTS, HIDDEN), BF16),
        ],
        compiler_params=pltpu.CompilerParams(vmem_limit_bytes=62 * 1024 * 1024),
        name="values",
    )(paths, mine, other, policy, value_in, value_out)


def on_device(frontier, policy_table, first, policy_index, owner_index, following, value_in, value_out):
    core = lax.axis_index("owner_3").astype(I32)[None]
    common, spec = tables(first, owner_index, policy_index, following)
    ranges = jnp.pad(frontier, ((0, 0), (0, WIDTH - HANDS))).reshape(FROWS, 128)
    shared = jnp.concatenate([ranges, common[:COMMON]], axis=0)
    block = jnp.concatenate(
        [jnp.broadcast_to(shared[None], (CHIPS,) + shared.shape), spec.reshape(CHIPS, 2, 128)], axis=1
    )
    mine = lax.all_to_all(block, OWNER[:3], split_axis=0, concat_axis=0, tiled=True)
    policy = jnp.pad(policy_table, ((0, 1), (0, WIDTH - HANDS))).astype(F32).reshape((POLICY + 1) * CHUNKS, 128)
    policy = jnp.pad(policy, ((0, 13), (0, 0)))
    weights_in = jnp.pad(value_in, ((0, WIDTH - HANDS), (0, 0)))
    mine, policy, weights_in = lax.optimization_barrier((mine, policy, weights_in))
    other = lax.ppermute(mine, OWNER[3], [(0, 1), (1, 0)])

    def part(x):
        return x[:, FROWS:, :].reshape(CHIPS * TROWS, 128)

    found = paths(core, part(mine), part(other))
    out = values(found, mine, other, policy, weights_in, jnp.transpose(value_out))
    return jnp.transpose(out, (0, 2, 1))


def solution(mesh):
    torus = Mesh(mesh.devices.reshape(4, 4, 4, 2), OWNER)
    placed = (P(OWNER, None), P(), P(OWNER), P(None, OWNER), P(None, OWNER), P(None, OWNER), P(), P())
    return jax.shard_map(on_device, mesh=torus, in_specs=placed, out_specs=P(None, OWNER, None), check_vma=False)
```

```python
import jax
import jax.numpy as jnp
from jax import lax
from jax.experimental import pallas as pl
from jax.experimental.pallas import tpu as pltpu
from jax.sharding import Mesh
from jax.sharding import PartitionSpec as P

HANDS = 1326
HIDDEN = 1536
POLICY = 2048
SLOTS = 512
DEVICES = 128
CHIPS = 64
FRONT = 16
CAP = 4
KEPT = 384 * DEVICES
CHUNKS = 11
WIDTH = CHUNKS * 128
FROWS = FRONT * CHUNKS
COMMON = 38
TROWS = COMMON + 2
BROWS = FROWS + TROWS
STRIDE = 17
UNROLL = 64
OWNER = ("owner_0", "owner_1", "owner_2", "owner_3")
F32 = jnp.float32
BF16 = jnp.bfloat16
I32 = jnp.int32


def iota(shape, dim):
    return lax.broadcasted_iota(I32, shape, dim)


def mm(a, b, dims):
    return lax.dot_general(a.astype(BF16), b.astype(BF16), (dims, ((), ())), preferred_element_type=F32)


NN = ((1,), (0,))
NT = ((1,), (1,))
TN = ((0,), (0,))


def tables_kernel(first_ref, owner_ref, policy_ref, next_ref, common_ref, spec_ref):
    lane = iota((1, SLOTS), 1)
    segment = jnp.zeros((1, SLOTS), I32)
    running = jnp.int32(0)
    for k in range(FRONT):
        running = running + first_ref[k]
        if k < FRONT - 1:
            segment = segment + (running <= lane).astype(I32)
    total = jnp.minimum(running, SLOTS)
    upper = (iota((SLOTS, SLOTS), 0) <= iota((SLOTS, SLOTS), 1)).astype(F32).astype(BF16)
    rows = []
    for level in range(3):
        hit = iota((DEVICES, SLOTS), 0) == owner_ref[level : level + 1, :]
        rank = mm(hit.astype(F32), upper, NN)
        policy = policy_ref[level : level + 1, :]
        fields = [lane - SLOTS // 2, jnp.ones_like(lane), lax.shift_right_logical(policy, 4), policy & 15]
        fields.append(next_ref[level : level + 1, :] if level < 2 else jnp.zeros_like(lane))
        fields.append(segment)
        values = jnp.concatenate(fields + [jnp.zeros_like(lane)] * 2, axis=0).astype(F32)
        found = []
        for r in range(CAP):
            mask = jnp.where(hit & (rank == r + 1), 1.0, 0.0)
            found.append(mm(values, mask, NT))
        slot = [f[0:1] + (SLOTS // 2) * (1.0 - f[1:2]) for f in found]
        high = [f[2:3] for f in found]
        low = [f[3:4] for f in found]
        count = [f[4:5] for f in found]
        parent = [f[5:6] for f in found]
        if level == 0:
            rows += slot + count + high + low + parent
        elif level == 1:
            rows += slot + count + high + low
        else:
            last = slot + high + low
    lanes = jnp.zeros((1, DEVICES), F32)
    zero = [lanes]
    common = rows + [lanes + (total - SLOTS // 2).astype(F32)] + zero
    common = jnp.concatenate(common + zero * (40 - len(common)), axis=0)
    common_ref[...] = common.astype(BF16)
    spec = jnp.concatenate(rows + last + zero * (DEVICES - len(rows) - len(last)), axis=0)
    spec_ref[...] = jnp.transpose(spec).astype(BF16)


def tables(first, owner, policy, following):
    vm = pl.BlockSpec(memory_space=pltpu.VMEM)
    return pl.pallas_call(
        tables_kernel,
        out_shape=[
            jax.ShapeDtypeStruct((40, DEVICES), BF16),
            jax.ShapeDtypeStruct((DEVICES, DEVICES), BF16),
        ],
        in_specs=[pl.BlockSpec(memory_space=pltpu.SMEM), vm, vm, vm],
        out_specs=[vm, vm],
        name="tables",
    )(first, owner, policy, following)


def follow(core, table_ref, out_ref, wide_ref):
    for h in range(2):
        for i in range(CHIPS):
            wide_ref[h, pl.ds(i * TROWS, TROWS), :] = table_ref[h, i].astype(F32)

    def field(h, row):
        return wide_ref[h, pl.ds(row, CHIPS, stride=TROWS), :]

    def full(base):
        return jnp.concatenate([field(h, base + r) for r in range(CAP) for h in range(2)], axis=0)

    n = 2 * CAP * CHIPS

    def places(shape, dim):
        i = iota(shape, dim)
        g, h, r = i & 63, lax.shift_right_logical(i, 6) & 1, lax.shift_right_logical(i, 7)
        return g, h, r, 2 * g + (h ^ core)

    def flag(x):
        return jnp.where(x, 1.0, 0.0).astype(BF16)

    half = SLOTS // 2
    g, h, r, s_row = places((n, DEVICES), 0)
    location = (h * CHIPS + g).astype(F32)
    s_f = s_row.astype(F32)
    s_loc_lane = 2 * (iota((n, DEVICES), 1) & 63) + (lax.shift_right_logical(iota((n, DEVICES), 1), 6) ^ core)
    lane = iota((n, DEVICES), 1)
    _, _, ra, sa = places((n, n), 0)
    _, _, rb, sb = places((n, n), 1)
    before = flag(sb * CAP + rb <= sa * CAP + ra)
    loc0 = iota((DEVICES, DEVICES), 0)
    s0 = 2 * (loc0 & 63) + (lax.shift_right_logical(loc0, 6) ^ core)
    d1 = iota((DEVICES, DEVICES), 1)
    turn = flag(s0 == d1)
    d_lane = iota((1, DEVICES), 1)
    d_f = d_lane.astype(F32)
    d_location = ((d_lane & 1) ^ core) * CHIPS + lax.shift_right_logical(d_lane, 1)

    spec = jnp.concatenate(
        [jnp.where(core == 0, field(k, COMMON), field(k, COMMON + 1)) for k in range(2)], axis=0
    )
    own = mm(spec, turn, TN)

    def mine(base):
        return own[base : base + CAP]

    totals = jnp.concatenate([field(0, 36), field(1, 36)], axis=0)
    offset = mm(flag(s_loc_lane < s_row), totals, NN) + half * s_f
    total = mm(flag(s_loc_lane == s_row), totals, NN) + half
    slot = full(0) + half
    kept = (slot < total) & (offset + slot < KEPT)
    count2 = jnp.where(kept, full(4), 0.0)
    cum2 = mm(before, count2, NN)
    ex2 = cum2 - count2
    total2 = jnp.minimum(jnp.sum(count2, axis=0, keepdims=True), float(SLOTS))
    total1_d = mm(totals, turn, TN)[0:1] + half
    offset1_d = mm(totals, flag(s0 < d1), TN)[0:1] + half * d_f
    j1 = mine(0) + half
    ok1 = (j1 < total1_d) & (offset1_d + j1 < KEPT)
    floc1 = d_location.astype(F32) * FRONT + mine(16)
    q1 = mine(8) * 16 + mine(12)
    wide2 = jnp.broadcast_to(total2 - half, (DEVICES, DEVICES))
    below = flag(loc0 < d1)
    less = flag(lane < s_row)
    same = flag(lane == s_row)
    offset = mm(less, wide2, NT) + half * s_f
    total = mm(same, wide2, NT) + half
    slot2 = full(20) + half
    kept = (slot2 < total) & (offset + slot2 < KEPT)
    count3 = jnp.where(kept, full(24), 0.0)
    cum3 = mm(before, count3, NN)
    ex3 = cum3 - count3
    total3 = jnp.minimum(jnp.sum(count3, axis=0, keepdims=True), float(SLOTS))
    j2 = mine(20) + half
    offset2_d = mm(wide2, below, NN)[0:1] + half * d_f
    ok2 = (j2 < total2) & (offset2_d + j2 < KEPT)
    parent1 = full(16)
    high1, low1 = full(8), full(12)
    path1 = (location * FRONT + parent1) * POLICY + high1 * 16 + low1
    path2 = []
    for r in range(CAP):
        j = j2[r : r + 1]
        path2.append(jnp.sum(jnp.where((ex2 <= j) & (j < cum2), path1, 0.0), axis=0, keepdims=True))
    path2 = jnp.concatenate(path2, axis=0).astype(I32)
    wide3 = jnp.broadcast_to(total3 - half, (DEVICES, DEVICES))
    offset3_d = mm(wide3, below, NN)[0:1] + half * d_f
    j3 = mine(36) + half
    ok3 = (j3 < total3) & (offset3_d + j3 < KEPT)
    policy2 = full(28) * 16 + full(32)
    via = s_f * 1024 + slot2
    stack = jnp.concatenate(
        [
            (jnp.minimum(cum2, float(SLOTS)) - half).astype(BF16),
            (jnp.minimum(ex2, float(SLOTS)) - half).astype(BF16),
            parent1.astype(BF16),
            high1.astype(BF16),
            low1.astype(BF16),
        ],
        axis=0,
    )
    path3, policy3 = [], []
    for r in range(CAP):
        j = j3[r : r + 1]
        hit = (ex3 <= j) & (j < cum3)
        policy3.append(jnp.sum(jnp.where(hit, policy2, 0.0), axis=0, keepdims=True))
        through = jnp.sum(jnp.where(hit, via, 0.0), axis=0, keepdims=True).astype(I32)
        device = lax.shift_right_logical(through, 10)
        jj = (through & 1023).astype(F32) - half
        got = mm(stack, flag(loc0 == device), NN)
        hit = (got[n : 2 * n] <= jj) & (jj < got[:n])
        path = (location * FRONT + got[2 * n : 3 * n]) * POLICY + got[3 * n : 4 * n] * 16 + got[4 * n :]
        path3.append(jnp.sum(jnp.where(hit, path, 0.0), axis=0, keepdims=True))
    path3 = jnp.concatenate(path3, axis=0).astype(I32)
    policy3 = jnp.concatenate(policy3, axis=0).astype(I32)

    def last(ok, base):
        return jnp.where(ok, (mine(base) * 16 + mine(base + 4)).astype(I32), POLICY)

    out_ref[0:4] = floc1.astype(I32)
    out_ref[4:8] = jnp.where(ok1, q1.astype(I32), POLICY)
    out_ref[8:12] = lax.shift_right_logical(path2, 11)
    out_ref[12:16] = path2 & (POLICY - 1)
    out_ref[16:20] = last(ok2, 28)
    out_ref[20:24] = lax.shift_right_logical(path3, 11)
    out_ref[24:28] = path3 & (POLICY - 1)
    out_ref[28:32] = policy3
    out_ref[32:36] = last(ok3, 40)
    out_ref[36:40] = jnp.zeros((4, DEVICES), I32)


FIELDS = ((0, (4,)), (8, (12, 16)), (20, (24, 28, 32)))


def values_kernel(
    core_ref,
    mine_ref,
    other_ref,
    policy_hbm,
    in_hbm,
    out_w_hbm,
    out_hbm,
    table_ref,
    wide_ref,
    found_ref,
    paths_ref,
    ranges_ref,
    front_ref,
    policy_ref,
    in_ref,
    out_w_ref,
    a_ref,
    b_ref,
    c_ref,
    y_ref,
    x0_ref,
    x1_ref,
    h_ref,
    v0_ref,
    v1_ref,
    sems,
):
    def load(src, dst, k):
        copy = pltpu.make_async_copy(src, dst, sems.at[k])
        copy.start()
        return copy

    halves = (mine_ref, other_ref)
    table_loads = [load(ref.at[:, pl.ds(FROWS, TROWS), :], table_ref.at[k], k) for k, ref in enumerate(halves)]
    range_loads = [load(ref.at[:, pl.ds(0, FROWS), :], ranges_ref.at[k], 2 + k) for k, ref in enumerate(halves)]
    policy_load = load(policy_hbm, policy_ref, 4)
    in_load = load(in_hbm, in_ref, 5)
    out_w_load = load(out_w_hbm, out_w_ref, 6)
    for copy in table_loads:
        copy.wait()
    follow(core_ref[0], table_ref, found_ref, wide_ref)
    found_copy = load(found_ref, paths_ref, 7)
    for half in range(2):
        range_loads[half].wait()

        @pl.loop(0, CHIPS)
        def _(i, half=half):
            at = pl.multiple_of((half * CHIPS + i) * FROWS, FROWS)
            front_ref[pl.ds(at, FROWS), :] = ranges_ref[half, i].astype(F32)

    found_copy.wait()
    policy_load.wait()

    def rows_of(table, index):
        at = index * CHUNKS
        return table[pl.ds(at, 8), :], table[pl.ds(at + 8, 8), :]

    def rounded(t):
        return t.astype(BF16).astype(F32)

    def chunk(ref, start, k):
        return ref[pl.ds(start * STRIDE + k, 8, stride=STRIDE), :]

    def form(level, first, x_ref):
        place, policies = FIELDS[level]
        hold = (a_ref, b_ref, c_ref)[: level + 1]
        s0 = first // CAP if isinstance(first, int) else lax.shift_right_logical(first, 2)
        for e in range(UNROLL):
            s, r = s0 + e // CAP, e % CAP
            for k, (base, ref) in enumerate(zip(policies, hold)):
                lo, hi = rows_of(policy_ref, paths_ref[base + r, s])
                if k == 0:
                    flo, fhi = rows_of(front_ref, paths_ref[place + r, s])
                    lo, hi = lo * flo, hi * fhi
                ref[e * STRIDE : e * STRIDE + 8, :] = lo
                ref[e * STRIDE + 8 : e * STRIDE + 16, :] = hi
        scales = [None] * (UNROLL // 8)
        for step, ref in enumerate(hold):
            masses = []
            for u in range(UNROLL // 8):
                at = slice(u * 8, u * 8 + 8)
                mass = None
                for k in range(CHUNKS):
                    term = chunk(ref, u * 8, k)
                    cut = slice(k * 128, (k + 1) * 128)
                    if step:
                        term = term * rounded(y_ref[at, cut] * scales[u])
                    y_ref[at, cut] = term
                    mass = term if mass is None else mass + term
                masses.append(mass)
            masses = [jnp.sum(m, axis=1, keepdims=True) for m in masses]
            scales = [jnp.where(m > 0, HANDS / m, 0.0) for m in masses]
        for u in range(UNROLL // 16):
            at = pl.multiple_of(first + u * 16, 16)
            for k in range(CHUNKS):
                cut = slice(k * 128, (k + 1) * 128)
                pair = [y_ref[u * 16 + v * 8 : u * 16 + v * 8 + 8, cut] * scales[2 * u + v] for v in range(2)]
                x_ref[pl.ds(at, 16), cut] = jnp.concatenate(pair, axis=0).astype(BF16)

    @pl.loop(0, SLOTS // UNROLL)
    def _(i):
        form(0, i * UNROLL, x0_ref)

    xs, vs, stores = (x0_ref, x1_ref), (v0_ref, v1_ref), [None, None]
    in_load.wait()
    out_w_load.wait()
    for level in range(3):
        x_ref, v_ref, ahead = xs[level % 2], vs[level % 2], xs[(level + 1) % 2]
        if stores[level % 2] is not None:
            stores[level % 2].wait()

        for i in range(3):
            if level < 2:
                form(level + 1, i * UNROLL, ahead)
            cut = slice(i * 512, i * 512 + 512)
            hidden = jnp.dot(x_ref[...], in_ref[:, cut], preferred_element_type=F32)
            h_ref[:, cut] = jnp.maximum(hidden, 0.0).astype(BF16)

        def second(cut, v_ref=v_ref):
            value = lax.dot_general(out_w_ref[cut, :], h_ref[...], (NT, ((), ())), preferred_element_type=F32)
            v_ref[cut, :] = value.astype(BF16)

        for i in range(5):
            if level < 2:
                form(level + 1, (i + 3) * UNROLL, ahead)
            second(slice(i * 256, i * 256 + 256))

        second(slice(1280, HANDS))
        stores[level % 2] = load(v_ref, out_hbm.at[level], 8 + level % 2)
    for copy in stores:
        copy.wait()


def values(core, mine, other, policy, value_in, value_out):
    hbm = pl.BlockSpec(memory_space=pl.ANY)
    hold = pltpu.VMEM((UNROLL * STRIDE + 16, 128), F32)
    return pl.pallas_call(
        values_kernel,
        out_shape=jax.ShapeDtypeStruct((3, HANDS, SLOTS), BF16),
        in_specs=[pl.BlockSpec(memory_space=pltpu.SMEM), hbm, hbm, hbm, hbm, hbm],
        out_specs=hbm,
        scratch_shapes=[
            pltpu.VMEM((2, CHIPS, TROWS, 128), BF16),
            pltpu.VMEM((2, CHIPS * TROWS, 128), F32),
            pltpu.VMEM((40, 128), I32),
            pltpu.SMEM((40, 128), I32),
            pltpu.VMEM((2, CHIPS, FROWS, 128), BF16),
            pltpu.VMEM((DEVICES * FROWS + 8, 128), F32),
            pltpu.VMEM(policy.shape, F32),
            pltpu.VMEM((WIDTH, HIDDEN), BF16),
            pltpu.VMEM((HANDS, HIDDEN), BF16),
            hold,
            hold,
            hold,
            pltpu.VMEM((UNROLL, WIDTH), F32),
            pltpu.VMEM((SLOTS, WIDTH), BF16),
            pltpu.VMEM((SLOTS, WIDTH), BF16),
            pltpu.VMEM((SLOTS, HIDDEN), BF16),
            pltpu.VMEM((HANDS, SLOTS), BF16),
            pltpu.VMEM((HANDS, SLOTS), BF16),
            pltpu.SemaphoreType.DMA((10,)),
        ],
        compiler_params=pltpu.CompilerParams(vmem_limit_bytes=62 * 1024 * 1024),
        name="values",
    )(core, mine, other, policy, value_in, value_out)


def on_device(frontier, policy_table, first, policy_index, owner_index, following, value_in, value_out):
    core = lax.axis_index("owner_3").astype(I32)[None]
    common, spec = tables(first, owner_index, policy_index, following)
    ranges = jnp.pad(frontier, ((0, 0), (0, WIDTH - HANDS))).reshape(FROWS, 128)
    shared = jnp.concatenate([ranges, common[:COMMON]], axis=0)
    block = jnp.concatenate(
        [jnp.broadcast_to(shared[None], (CHIPS,) + shared.shape), spec.reshape(CHIPS, 2, 128)], axis=1
    )
    mine = lax.all_to_all(block, OWNER[:3], split_axis=0, concat_axis=0, tiled=True)
    policy = jnp.pad(policy_table, ((0, 1), (0, WIDTH - HANDS))).astype(F32).reshape((POLICY + 1) * CHUNKS, 128)
    policy = jnp.pad(policy, ((0, 13), (0, 0)))
    weights_in = jnp.pad(value_in, ((0, WIDTH - HANDS), (0, 0)))
    mine, policy, weights_in = lax.optimization_barrier((mine, policy, weights_in))
    other = lax.ppermute(mine, OWNER[3], [(0, 1), (1, 0)])

    out = values(core, mine, other, policy, weights_in, jnp.transpose(value_out))
    return jnp.transpose(out, (0, 2, 1))


def solution(mesh):
    torus = Mesh(mesh.devices.reshape(4, 4, 4, 2), OWNER)
    placed = (P(OWNER, None), P(), P(OWNER), P(None, OWNER), P(None, OWNER), P(None, OWNER), P(), P())
    return jax.shard_map(on_device, mesh=torus, in_specs=placed, out_specs=P(None, OWNER, None), check_vma=False)
```

```python
import jax
import jax.numpy as jnp
from jax import lax
from jax.experimental import pallas as pl
from jax.experimental.pallas import tpu as pltpu
from jax.sharding import Mesh
from jax.sharding import PartitionSpec as P

HANDS = 1326
HIDDEN = 1536
POLICY = 2048
SLOTS = 512
DEVICES = 128
CHIPS = 64
FRONT = 16
CAP = 4
KEPT = 384 * DEVICES
CHUNKS = 11
WIDTH = CHUNKS * 128
FROWS = FRONT * (CHUNKS - 1) + FRONT // 2
COMMON = 32
TROWS = COMMON + 8
BROWS = FROWS + TROWS
STRIDE = 17
UNROLL = 64
OWNER = ("owner_0", "owner_1", "owner_2", "owner_3")
F32 = jnp.float32
BF16 = jnp.bfloat16
I32 = jnp.int32


def iota(shape, dim):
    return lax.broadcasted_iota(I32, shape, dim)


def mm(a, b, dims):
    return lax.dot_general(a.astype(BF16), b.astype(BF16), (dims, ((), ())), preferred_element_type=F32)


NN = ((1,), (0,))
NT = ((1,), (1,))
TN = ((0,), (0,))


def tables_kernel(first_ref, owner_ref, policy_ref, next_ref, frontier_ref, out_hbm, block_ref, turn_ref, spec_ref, send_ref, sems):
    for k in range(CHUNKS - 1):
        block_ref[k * FRONT : (k + 1) * FRONT, :] = frontier_ref[:, k * 128 : (k + 1) * 128]
    tail = frontier_ref[:, (CHUNKS - 1) * 128 :].astype(F32)
    tail = jnp.concatenate([tail, jnp.zeros((FRONT, WIDTH - HANDS - 64), F32)], axis=1)
    tail = jnp.concatenate([tail[:8], tail[8:]], axis=1)
    lane = iota((1, SLOTS), 1)
    wide = iota((1, 128), 1)
    segment = jnp.zeros((1, SLOTS), I32)
    ends = jnp.zeros((1, 128), I32)
    running = jnp.int32(0)
    for k in range(FRONT):
        running = running + first_ref[k]
        ends = jnp.where(wide == 64 + k, jnp.minimum(running, SLOTS) - SLOTS // 2, ends)
        if k < FRONT - 1:
            segment = segment + (running <= lane).astype(I32)
    ends = jnp.where(wide == 80, jnp.minimum(running, SLOTS) - SLOTS // 2, ends)
    upper = (iota((SLOTS, SLOTS), 0) <= iota((SLOTS, SLOTS), 1)).astype(F32).astype(BF16)
    rows, own = [], []
    for level in range(3):
        hit = iota((DEVICES, SLOTS), 0) == owner_ref[level : level + 1, :]
        rank = mm(hit.astype(F32), upper, NN)
        policy = policy_ref[level : level + 1, :]
        fields = [lane - SLOTS // 2, jnp.ones_like(lane), lax.shift_right_logical(policy, 4), policy & 15]
        fields.append(next_ref[level : level + 1, :] if level < 2 else jnp.zeros_like(lane))
        fields.append(segment)
        values = jnp.concatenate(fields + [jnp.zeros_like(lane)] * 2, axis=0).astype(F32)
        found = []
        for r in range(CAP):
            mask = jnp.where(hit & (rank == r + 1), 1.0, 0.0)
            found.append(mm(values, mask, NT))
        slot = [f[0:1] + (SLOTS // 2) * (1.0 - f[1:2]) for f in found]
        high = [f[2:3] for f in found]
        low = [f[3:4] for f in found]
        count = [f[4:5] for f in found]
        parent = [f[5:6] for f in found]
        if level < 2:
            rows += slot + count + high + low
        own += slot + high + low + (parent if level == 0 else [])
    block_ref[FROWS - 8 :, :] = jnp.concatenate([tail] + rows, axis=0).astype(BF16)
    copies = [
        pltpu.make_async_copy(block_ref, out_hbm.at[i, pl.ds(0, FROWS + COMMON), :], sems.at[0]) for i in range(CHIPS)
    ]
    for copy in copies:
        copy.start()
    zero = [jnp.zeros((1, DEVICES), F32)]
    turn_ref[...] = jnp.transpose(jnp.concatenate(own + zero * (DEVICES - len(own)), axis=0)) + ends.astype(F32)
    spec_ref[...] = jnp.zeros((CHIPS * 8, 128), F32)
    for c in range(2):
        spec_ref[pl.ds(c, CHIPS, stride=8), :] = turn_ref[pl.ds(c, CHIPS, stride=2), :]
    send_ref[...] = spec_ref[...].astype(BF16).reshape(CHIPS, 8, 128)
    last = pltpu.make_async_copy(send_ref, out_hbm.at[:, pl.ds(FROWS + COMMON, 8), :], sems.at[1])
    last.start()
    for copy in copies:
        copy.wait()
    last.wait()


def tables(first, owner, policy, following, frontier):
    vm = pl.BlockSpec(memory_space=pltpu.VMEM)
    return pl.pallas_call(
        tables_kernel,
        out_shape=jax.ShapeDtypeStruct((CHIPS, BROWS, 128), BF16),
        in_specs=[pl.BlockSpec(memory_space=pltpu.SMEM), vm, vm, vm, vm],
        out_specs=pl.BlockSpec(memory_space=pl.ANY),
        scratch_shapes=[
            pltpu.VMEM((FROWS + COMMON, 128), BF16),
            pltpu.VMEM((DEVICES, 128), F32),
            pltpu.VMEM((CHIPS * 8, 128), F32),
            pltpu.VMEM((CHIPS, 8, 128), BF16),
            pltpu.SemaphoreType.DMA((2,)),
        ],
        name="tables",
    )(first, owner, policy, following, frontier)


def follow(core, table_ref, out_ref, wide_ref):
    for h in range(2):
        for i in range(CHIPS):
            wide_ref[h, pl.ds(i * TROWS, TROWS), :] = table_ref[h, i].astype(F32)

    def field(h, row):
        return wide_ref[h, pl.ds(row, CHIPS, stride=TROWS), :]

    def full(base):
        return jnp.concatenate([field(h, base + r) for r in range(CAP) for h in range(2)], axis=0)

    n = 2 * CAP * CHIPS

    def places(shape, dim):
        i = iota(shape, dim)
        g, h, r = i & 63, lax.shift_right_logical(i, 6) & 1, lax.shift_right_logical(i, 7)
        return g, h, r, 2 * g + (h ^ core)

    def flag(x):
        return jnp.where(x, 1.0, 0.0).astype(BF16)

    half = SLOTS // 2
    g, h, r, s_row = places((n, DEVICES), 0)
    location = (h * CHIPS + g).astype(F32)
    s_f = s_row.astype(F32)
    s_loc_lane = 2 * (iota((n, DEVICES), 1) & 63) + (lax.shift_right_logical(iota((n, DEVICES), 1), 6) ^ core)
    lane = iota((n, DEVICES), 1)
    _, _, ra, sa = places((n, n), 0)
    _, _, rb, sb = places((n, n), 1)
    before = flag(sb * CAP + rb <= sa * CAP + ra)
    loc0 = iota((DEVICES, DEVICES), 0)
    s0 = 2 * (loc0 & 63) + (lax.shift_right_logical(loc0, 6) ^ core)
    d1 = iota((DEVICES, DEVICES), 1)
    turn = flag(s0 == d1)
    d_lane = iota((1, DEVICES), 1)
    d_f = d_lane.astype(F32)
    d_location = ((d_lane & 1) ^ core) * CHIPS + lax.shift_right_logical(d_lane, 1)

    spec = jnp.concatenate(
        [jnp.where(core == 0, field(k, COMMON), field(k, COMMON + 1)) for k in range(2)], axis=0
    )
    own = mm(spec, turn, TN)

    def mine(base):
        return own[base : base + CAP]

    totals = jnp.broadcast_to(spec[:, 80:81], (DEVICES, DEVICES))
    offset = mm(flag(s_loc_lane < s_row), totals, NN) + half * s_f
    total = mm(flag(s_loc_lane == s_row), totals, NN) + half
    slot1 = full(0)
    parent1 = jnp.zeros((n, DEVICES), F32)
    for k in range(FRONT - 1):
        ends = jnp.broadcast_to(spec[:, 64 + k : 65 + k], (DEVICES, DEVICES))
        parent1 = parent1 + jnp.where(jnp.concatenate([ends] * CAP, axis=0) <= slot1, 1.0, 0.0)
    slot = slot1 + half
    kept = (slot < total) & (offset + slot < KEPT)
    count2 = jnp.where(kept, full(4), 0.0)
    cum2 = mm(before, count2, NN)
    ex2 = cum2 - count2
    total2 = jnp.minimum(jnp.sum(count2, axis=0, keepdims=True), float(SLOTS))
    total1_d = mm(totals, turn, TN)[0:1] + half
    offset1_d = mm(totals, flag(s0 < d1), TN)[0:1] + half * d_f
    j1 = mine(0) + half
    ok1 = (j1 < total1_d) & (offset1_d + j1 < KEPT)
    floc1 = d_location.astype(F32) * FRONT + mine(12)
    q1 = mine(4) * 16 + mine(8)
    wide2 = jnp.broadcast_to(total2 - half, (DEVICES, DEVICES))
    below = flag(loc0 < d1)
    less = flag(lane < s_row)
    same = flag(lane == s_row)
    offset = mm(less, wide2, NT) + half * s_f
    total = mm(same, wide2, NT) + half
    slot2 = full(16) + half
    kept = (slot2 < total) & (offset + slot2 < KEPT)
    count3 = jnp.where(kept, full(20), 0.0)
    cum3 = mm(before, count3, NN)
    ex3 = cum3 - count3
    total3 = jnp.minimum(jnp.sum(count3, axis=0, keepdims=True), float(SLOTS))
    j2 = mine(16) + half
    offset2_d = mm(wide2, below, NN)[0:1] + half * d_f
    ok2 = (j2 < total2) & (offset2_d + j2 < KEPT)
    high1, low1 = full(8), full(12)
    path1 = (location * FRONT + parent1) * POLICY + high1 * 16 + low1
    path2 = []
    for r in range(CAP):
        j = j2[r : r + 1]
        path2.append(jnp.sum(jnp.where((ex2 <= j) & (j < cum2), path1, 0.0), axis=0, keepdims=True))
    path2 = jnp.concatenate(path2, axis=0).astype(I32)
    wide3 = jnp.broadcast_to(total3 - half, (DEVICES, DEVICES))
    offset3_d = mm(wide3, below, NN)[0:1] + half * d_f
    j3 = mine(28) + half
    ok3 = (j3 < total3) & (offset3_d + j3 < KEPT)
    policy2 = full(24) * 16 + full(28)
    via = s_f * 1024 + slot2
    stack = jnp.concatenate(
        [
            (jnp.minimum(cum2, float(SLOTS)) - half).astype(BF16),
            (jnp.minimum(ex2, float(SLOTS)) - half).astype(BF16),
            parent1.astype(BF16),
            high1.astype(BF16),
            low1.astype(BF16),
        ],
        axis=0,
    )
    path3, policy3 = [], []
    for r in range(CAP):
        j = j3[r : r + 1]
        hit = (ex3 <= j) & (j < cum3)
        policy3.append(jnp.sum(jnp.where(hit, policy2, 0.0), axis=0, keepdims=True))
        through = jnp.sum(jnp.where(hit, via, 0.0), axis=0, keepdims=True).astype(I32)
        device = lax.shift_right_logical(through, 10)
        jj = (through & 1023).astype(F32) - half
        got = mm(stack, flag(loc0 == device), NN)
        hit = (got[n : 2 * n] <= jj) & (jj < got[:n])
        path = (location * FRONT + got[2 * n : 3 * n]) * POLICY + got[3 * n : 4 * n] * 16 + got[4 * n :]
        path3.append(jnp.sum(jnp.where(hit, path, 0.0), axis=0, keepdims=True))
    path3 = jnp.concatenate(path3, axis=0).astype(I32)
    policy3 = jnp.concatenate(policy3, axis=0).astype(I32)

    def last(ok, base):
        return jnp.where(ok, (mine(base) * 16 + mine(base + 4)).astype(I32), POLICY)

    out_ref[0:4] = floc1.astype(I32)
    out_ref[4:8] = jnp.where(ok1, q1.astype(I32), POLICY)
    out_ref[8:12] = lax.shift_right_logical(path2, 11)
    out_ref[12:16] = path2 & (POLICY - 1)
    out_ref[16:20] = last(ok2, 20)
    out_ref[20:24] = lax.shift_right_logical(path3, 11)
    out_ref[24:28] = path3 & (POLICY - 1)
    out_ref[28:32] = policy3
    out_ref[32:36] = last(ok3, 32)
    out_ref[36:40] = jnp.zeros((4, DEVICES), I32)


FIELDS = ((0, (4,)), (8, (12, 16)), (20, (24, 28, 32)))


def values_kernel(
    core_ref,
    mine_ref,
    other_ref,
    policy_hbm,
    in_hbm,
    out_w_hbm,
    out_hbm,
    table_ref,
    wide_ref,
    found_ref,
    paths_ref,
    ranges_ref,
    front_ref,
    policy_ref,
    in_ref,
    out_w_ref,
    a_ref,
    b_ref,
    c_ref,
    y_ref,
    x0_ref,
    x1_ref,
    h_ref,
    v0_ref,
    v1_ref,
    sems,
):
    def load(src, dst, k):
        copy = pltpu.make_async_copy(src, dst, sems.at[k])
        copy.start()
        return copy

    halves = (mine_ref, other_ref)
    table_loads = [load(ref.at[:, pl.ds(FROWS, TROWS), :], table_ref.at[k], k) for k, ref in enumerate(halves)]
    range_loads = [load(ref.at[:, pl.ds(0, FROWS), :], ranges_ref.at[k], 2 + k) for k, ref in enumerate(halves)]
    policy_load = load(policy_hbm, policy_ref, 4)
    in_load = load(in_hbm, in_ref, 5)
    out_w_load = load(out_w_hbm, out_w_ref, 6)
    for copy in table_loads:
        copy.wait()
    follow(core_ref[0], table_ref, found_ref, wide_ref)
    found_copy = load(found_ref, paths_ref, 7)
    for half in range(2):
        range_loads[half].wait()

        @pl.loop(0, CHIPS // 16)
        def _(j, half=half):
            for e in range(16):
                i = j * 16 + e
                at = (half * CHIPS + i) * (FRONT * CHUNKS)
                for k in range(CHUNKS - 1):
                    wide = ranges_ref[half, i, k * FRONT : (k + 1) * FRONT].astype(F32)
                    front_ref[pl.ds(at + k, FRONT, stride=CHUNKS), :] = wide
                tail = ranges_ref[half, i, FROWS - 8 : FROWS].astype(F32)
                front_ref[pl.ds(at + CHUNKS - 1, 8, stride=CHUNKS), :] = tail
                front_ref[pl.ds(at + 9 * CHUNKS - 1, 8, stride=CHUNKS), :] = pltpu.roll(tail, 64, 1)

    found_copy.wait()
    policy_load.wait()

    def rows_of(table, index):
        at = index * CHUNKS
        return table[pl.ds(at, 8), :], table[pl.ds(at + 8, 8), :]

    def rounded(t):
        return t.astype(BF16).astype(F32)

    def chunk(ref, start, k):
        return ref[pl.ds(start * STRIDE + k, 8, stride=STRIDE), :]

    def form(level, first, x_ref):
        place, policies = FIELDS[level]
        hold = (a_ref, b_ref, c_ref)[: level + 1]
        s0 = first // CAP if isinstance(first, int) else lax.shift_right_logical(first, 2)
        for e in range(UNROLL):
            s, r = s0 + e // CAP, e % CAP
            for k, (base, ref) in enumerate(zip(policies, hold)):
                lo, hi = rows_of(policy_ref, paths_ref[base + r, s])
                if k == 0:
                    flo, fhi = rows_of(front_ref, paths_ref[place + r, s])
                    lo, hi = lo * flo, hi * fhi
                ref[e * STRIDE : e * STRIDE + 8, :] = lo
                ref[e * STRIDE + 8 : e * STRIDE + 16, :] = hi
        scales = [None] * (UNROLL // 8)
        for step, ref in enumerate(hold):
            masses = []
            for u in range(UNROLL // 8):
                at = slice(u * 8, u * 8 + 8)
                mass = None
                for k in range(CHUNKS):
                    term = chunk(ref, u * 8, k)
                    cut = slice(k * 128, (k + 1) * 128)
                    if step:
                        term = term * rounded(y_ref[at, cut] * scales[u])
                    y_ref[at, cut] = term
                    mass = term if mass is None else mass + term
                masses.append(mass)
            masses = [jnp.sum(m, axis=1, keepdims=True) for m in masses]
            scales = [jnp.where(m > 0, HANDS / m, 0.0) for m in masses]
        for u in range(UNROLL // 16):
            at = pl.multiple_of(first + u * 16, 16)
            for k in range(CHUNKS):
                cut = slice(k * 128, (k + 1) * 128)
                pair = [y_ref[u * 16 + v * 8 : u * 16 + v * 8 + 8, cut] * scales[2 * u + v] for v in range(2)]
                x_ref[pl.ds(at, 16), cut] = jnp.concatenate(pair, axis=0).astype(BF16)

    @pl.loop(0, SLOTS // UNROLL)
    def _(i):
        form(0, i * UNROLL, x0_ref)

    xs, vs, stores = (x0_ref, x1_ref), (v0_ref, v1_ref), [None, None]
    in_load.wait()
    out_w_load.wait()
    for level in range(3):
        x_ref, v_ref, ahead = xs[level % 2], vs[level % 2], xs[(level + 1) % 2]
        if stores[level % 2] is not None:
            stores[level % 2].wait()

        for i in range(3):
            if level < 2:
                form(level + 1, i * UNROLL, ahead)
            cut = slice(i * 512, i * 512 + 512)
            hidden = jnp.dot(x_ref[...], in_ref[:, cut], preferred_element_type=F32)
            h_ref[:, cut] = jnp.maximum(hidden, 0.0).astype(BF16)

        def second(cut, v_ref=v_ref):
            value = lax.dot_general(out_w_ref[cut, :], h_ref[...], (NT, ((), ())), preferred_element_type=F32)
            v_ref[cut, :] = value.astype(BF16)

        for i in range(5):
            if level < 2:
                form(level + 1, (i + 3) * UNROLL, ahead)
            second(slice(i * 256, i * 256 + 256))

        second(slice(1280, HANDS))
        stores[level % 2] = load(v_ref, out_hbm.at[level], 8 + level % 2)
    for copy in stores:
        copy.wait()


def values(core, mine, other, policy, value_in, value_out):
    hbm = pl.BlockSpec(memory_space=pl.ANY)
    hold = pltpu.VMEM((UNROLL * STRIDE + 16, 128), F32)
    return pl.pallas_call(
        values_kernel,
        out_shape=jax.ShapeDtypeStruct((3, HANDS, SLOTS), BF16),
        in_specs=[pl.BlockSpec(memory_space=pltpu.SMEM), hbm, hbm, hbm, hbm, hbm],
        out_specs=hbm,
        scratch_shapes=[
            pltpu.VMEM((2, CHIPS, TROWS, 128), BF16),
            pltpu.VMEM((2, CHIPS * TROWS, 128), F32),
            pltpu.VMEM((40, 128), I32),
            pltpu.SMEM((40, 128), I32),
            pltpu.VMEM((2, CHIPS, FROWS, 128), BF16),
            pltpu.VMEM((DEVICES * FRONT * CHUNKS + 8, 128), F32),
            pltpu.VMEM(policy.shape, F32),
            pltpu.VMEM((WIDTH, HIDDEN), BF16),
            pltpu.VMEM((HANDS, HIDDEN), BF16),
            hold,
            hold,
            hold,
            pltpu.VMEM((UNROLL, WIDTH), F32),
            pltpu.VMEM((SLOTS, WIDTH), BF16),
            pltpu.VMEM((SLOTS, WIDTH), BF16),
            pltpu.VMEM((SLOTS, HIDDEN), BF16),
            pltpu.VMEM((HANDS, SLOTS), BF16),
            pltpu.VMEM((HANDS, SLOTS), BF16),
            pltpu.SemaphoreType.DMA((10,)),
        ],
        compiler_params=pltpu.CompilerParams(vmem_limit_bytes=62 * 1024 * 1024),
        name="values",
    )(core, mine, other, policy, value_in, value_out)


def on_device(frontier, policy_table, first, policy_index, owner_index, following, value_in, value_out):
    core = lax.axis_index("owner_3").astype(I32)[None]
    block = tables(first, owner_index, policy_index, following, frontier)
    mine = lax.all_to_all(block, OWNER[:3], split_axis=0, concat_axis=0, tiled=True)
    policy = jnp.pad(policy_table, ((0, 1), (0, WIDTH - HANDS))).astype(F32).reshape((POLICY + 1) * CHUNKS, 128)
    policy = jnp.pad(policy, ((0, 13), (0, 0)))
    weights_in = jnp.pad(value_in, ((0, WIDTH - HANDS), (0, 0)))
    mine, policy, weights_in = lax.optimization_barrier((mine, policy, weights_in))
    other = lax.ppermute(mine, OWNER[3], [(0, 1), (1, 0)])

    out = values(core, mine, other, policy, weights_in, jnp.transpose(value_out))
    return jnp.transpose(out, (0, 2, 1))


def solution(mesh):
    torus = Mesh(mesh.devices.reshape(4, 4, 4, 2), OWNER)
    placed = (P(OWNER, None), P(), P(OWNER), P(None, OWNER), P(None, OWNER), P(None, OWNER), P(), P())
    return jax.shard_map(on_device, mesh=torus, in_specs=placed, out_specs=P(None, OWNER, None), check_vma=False)
```

```python
import jax
import jax.numpy as jnp
from jax import lax
from jax.experimental import pallas as pl
from jax.experimental.pallas import tpu as pltpu
from jax.sharding import Mesh
from jax.sharding import PartitionSpec as P

HANDS = 1326
HIDDEN = 1536
POLICY = 2048
SLOTS = 512
DEVICES = 128
CHIPS = 64
FRONT = 16
CAP = 4
KEPT = 384 * DEVICES
CHUNKS = 11
WIDTH = CHUNKS * 128
FROWS = FRONT * (CHUNKS - 1)
COMMON = 32
ENDS = 44
PIECE = 18
SPARE = (46, 110)
TROWS = COMMON + 8
BROWS = FROWS + TROWS
STRIDE = 17
UNROLL = 64
OWNER = ("owner_0", "owner_1", "owner_2", "owner_3")
F32 = jnp.float32
BF16 = jnp.bfloat16
I32 = jnp.int32


def iota(shape, dim):
    return lax.broadcasted_iota(I32, shape, dim)


def mm(a, b, dims):
    return lax.dot_general(a.astype(BF16), b.astype(BF16), (dims, ((), ())), preferred_element_type=F32)


NN = ((1,), (0,))
NT = ((1,), (1,))
TN = ((0,), (0,))


def tables_kernel(first_ref, owner_ref, policy_ref, next_ref, frontier_ref, out_hbm, block_ref, turn_ref, spec_ref, send_ref, sems):
    for k in range(CHUNKS - 1):
        block_ref[k * FRONT : (k + 1) * FRONT, :] = frontier_ref[:, k * 128 : (k + 1) * 128]
    tail = frontier_ref[:, (CHUNKS - 1) * 128 :].astype(F32)
    tail = jnp.concatenate([tail, jnp.zeros((FRONT, WIDTH - HANDS - 64), F32)], axis=1)
    tail = jnp.concatenate([tail[:8], tail[8:]], axis=1)
    lane = iota((1, SLOTS), 1)
    wide = iota((1, 128), 1)
    segment = jnp.zeros((1, SLOTS), I32)
    ends = jnp.zeros((1, 128), I32)
    running = jnp.int32(0)
    for k in range(FRONT):
        running = running + first_ref[k]
        ends = jnp.where(wide == ENDS + k, jnp.minimum(running, SLOTS) - SLOTS // 2, ends)
        if k < FRONT - 1:
            segment = segment + (running <= lane).astype(I32)
    ends = jnp.where(wide == ENDS + FRONT, jnp.minimum(running, SLOTS) - SLOTS // 2, ends)
    upper = (iota((SLOTS, SLOTS), 0) <= iota((SLOTS, SLOTS), 1)).astype(F32).astype(BF16)
    rows, own = [], []
    for level in range(3):
        hit = iota((DEVICES, SLOTS), 0) == owner_ref[level : level + 1, :]
        rank = mm(hit.astype(F32), upper, NN)
        policy = policy_ref[level : level + 1, :]
        fields = [lane - SLOTS // 2, jnp.ones_like(lane), lax.shift_right_logical(policy, 4), policy & 15]
        fields.append(next_ref[level : level + 1, :] if level < 2 else jnp.zeros_like(lane))
        fields.append(segment)
        values = jnp.concatenate(fields + [jnp.zeros_like(lane)] * 2, axis=0).astype(F32)
        found = []
        for r in range(CAP):
            mask = jnp.where(hit & (rank == r + 1), 1.0, 0.0)
            found.append(mm(values, mask, NT))
        slot = [f[0:1] + (SLOTS // 2) * (1.0 - f[1:2]) for f in found]
        high = [f[2:3] for f in found]
        low = [f[3:4] for f in found]
        count = [f[4:5] for f in found]
        parent = [f[5:6] for f in found]
        if level < 2:
            rows += slot + count + high + low
        own += slot + high + low + (parent if level == 0 else [])
    block_ref[FROWS:, :] = jnp.concatenate(rows, axis=0).astype(BF16)
    copies = [
        pltpu.make_async_copy(block_ref, out_hbm.at[i, pl.ds(0, FROWS + COMMON), :], sems.at[0]) for i in range(CHIPS)
    ]
    for copy in copies:
        copy.start()
    zero = [jnp.zeros((1, DEVICES), F32)]
    turn_ref[...] = jnp.transpose(jnp.concatenate(own + zero * (DEVICES - len(own)), axis=0)) + ends.astype(F32)
    turned = turn_ref[...]
    lanes = iota((DEVICES, 128), 1)
    spec_ref[...] = jnp.broadcast_to(tail[None], (CHIPS, 8, 128)).reshape(CHIPS * 8, 128)
    for j in range(2):
        left = pltpu.roll(turned, (SPARE[0] - 2 * j * PIECE) % 128, 1)
        right = pltpu.roll(turned, (SPARE[1] - (2 * j + 1) * PIECE) % 128, 1)
        left = jnp.where((lanes >= SPARE[0]) & (lanes < SPARE[0] + PIECE), left, 0.0)
        turn_ref[...] = left + jnp.where(lanes >= SPARE[1], right, 0.0)
        for c in range(2):
            at = pl.ds(2 * c + j, CHIPS, stride=8)
            spec_ref[at, :] = spec_ref[at, :] + turn_ref[pl.ds(c, CHIPS, stride=2), :]
    send_ref[...] = spec_ref[...].astype(BF16).reshape(CHIPS, 8, 128)
    last = pltpu.make_async_copy(send_ref, out_hbm.at[:, pl.ds(FROWS + COMMON, 8), :], sems.at[1])
    last.start()
    for copy in copies:
        copy.wait()
    last.wait()


def tables(first, owner, policy, following, frontier):
    vm = pl.BlockSpec(memory_space=pltpu.VMEM)
    return pl.pallas_call(
        tables_kernel,
        out_shape=jax.ShapeDtypeStruct((CHIPS, BROWS, 128), BF16),
        in_specs=[pl.BlockSpec(memory_space=pltpu.SMEM), vm, vm, vm, vm],
        out_specs=pl.BlockSpec(memory_space=pl.ANY),
        scratch_shapes=[
            pltpu.VMEM((FROWS + COMMON, 128), BF16),
            pltpu.VMEM((DEVICES, 128), F32),
            pltpu.VMEM((CHIPS * 8, 128), F32),
            pltpu.VMEM((CHIPS, 8, 128), BF16),
            pltpu.SemaphoreType.DMA((2,)),
        ],
        name="tables",
    )(first, owner, policy, following, frontier)


def follow(core, table_ref, out_ref, wide_ref):
    for h in range(2):
        for i in range(CHIPS):
            wide_ref[h, pl.ds(i * TROWS, TROWS), :] = table_ref[h, i].astype(F32)

    def field(h, row):
        return wide_ref[h, pl.ds(row, CHIPS, stride=TROWS), :]

    def full(base):
        return jnp.concatenate([field(h, base + r) for r in range(CAP) for h in range(2)], axis=0)

    n = 2 * CAP * CHIPS

    def places(shape, dim):
        i = iota(shape, dim)
        g, h, r = i & 63, lax.shift_right_logical(i, 6) & 1, lax.shift_right_logical(i, 7)
        return g, h, r, 2 * g + (h ^ core)

    def flag(x):
        return jnp.where(x, 1.0, 0.0).astype(BF16)

    half = SLOTS // 2
    g, h, r, s_row = places((n, DEVICES), 0)
    location = (h * CHIPS + g).astype(F32)
    s_f = s_row.astype(F32)
    s_loc_lane = 2 * (iota((n, DEVICES), 1) & 63) + (lax.shift_right_logical(iota((n, DEVICES), 1), 6) ^ core)
    lane = iota((n, DEVICES), 1)
    _, _, ra, sa = places((n, n), 0)
    _, _, rb, sb = places((n, n), 1)
    before = flag(sb * CAP + rb <= sa * CAP + ra)
    loc0 = iota((DEVICES, DEVICES), 0)
    s0 = 2 * (loc0 & 63) + (lax.shift_right_logical(loc0, 6) ^ core)
    d1 = iota((DEVICES, DEVICES), 1)
    turn = flag(s0 == d1)
    d_lane = iota((1, DEVICES), 1)
    d_f = d_lane.astype(F32)
    d_location = ((d_lane & 1) ^ core) * CHIPS + lax.shift_right_logical(d_lane, 1)

    spec = jnp.zeros((DEVICES, DEVICES), F32)
    for j in range(2):
        row = [jnp.where(core == 0, field(k, COMMON + j), field(k, COMMON + 2 + j)) for k in range(2)]
        row = jnp.concatenate(row, axis=0)
        for e in range(2):
            piece = 2 * j + e
            back = pltpu.roll(row, (piece * PIECE - SPARE[e]) % 128, 1)
            spec = jnp.where((d1 >= piece * PIECE) & (d1 < (piece + 1) * PIECE), back, spec)
    own = mm(spec, turn, TN)

    def mine(base):
        return own[base : base + CAP]

    totals = jnp.broadcast_to(spec[:, ENDS + FRONT : ENDS + FRONT + 1], (DEVICES, DEVICES))
    offset = mm(flag(s_loc_lane < s_row), totals, NN) + half * s_f
    total = mm(flag(s_loc_lane == s_row), totals, NN) + half
    slot1 = full(0)
    parent1 = jnp.zeros((n, DEVICES), F32)
    for k in range(FRONT - 1):
        ends = jnp.broadcast_to(spec[:, ENDS + k : ENDS + k + 1], (DEVICES, DEVICES))
        parent1 = parent1 + jnp.where(jnp.concatenate([ends] * CAP, axis=0) <= slot1, 1.0, 0.0)
    slot = slot1 + half
    kept = (slot < total) & (offset + slot < KEPT)
    count2 = jnp.where(kept, full(4), 0.0)
    cum2 = mm(before, count2, NN)
    ex2 = cum2 - count2
    total2 = jnp.minimum(jnp.sum(count2, axis=0, keepdims=True), float(SLOTS))
    total1_d = mm(totals, turn, TN)[0:1] + half
    offset1_d = mm(totals, flag(s0 < d1), TN)[0:1] + half * d_f
    j1 = mine(0) + half
    ok1 = (j1 < total1_d) & (offset1_d + j1 < KEPT)
    floc1 = d_location.astype(F32) * FRONT + mine(12)
    q1 = mine(4) * 16 + mine(8)
    wide2 = jnp.broadcast_to(total2 - half, (DEVICES, DEVICES))
    below = flag(loc0 < d1)
    less = flag(lane < s_row)
    same = flag(lane == s_row)
    offset = mm(less, wide2, NT) + half * s_f
    total = mm(same, wide2, NT) + half
    slot2 = full(16) + half
    kept = (slot2 < total) & (offset + slot2 < KEPT)
    count3 = jnp.where(kept, full(20), 0.0)
    cum3 = mm(before, count3, NN)
    ex3 = cum3 - count3
    total3 = jnp.minimum(jnp.sum(count3, axis=0, keepdims=True), float(SLOTS))
    j2 = mine(16) + half
    offset2_d = mm(wide2, below, NN)[0:1] + half * d_f
    ok2 = (j2 < total2) & (offset2_d + j2 < KEPT)
    high1, low1 = full(8), full(12)
    path1 = (location * FRONT + parent1) * POLICY + high1 * 16 + low1
    path2 = []
    for r in range(CAP):
        j = j2[r : r + 1]
        path2.append(jnp.sum(jnp.where((ex2 <= j) & (j < cum2), path1, 0.0), axis=0, keepdims=True))
    path2 = jnp.concatenate(path2, axis=0).astype(I32)
    wide3 = jnp.broadcast_to(total3 - half, (DEVICES, DEVICES))
    offset3_d = mm(wide3, below, NN)[0:1] + half * d_f
    j3 = mine(28) + half
    ok3 = (j3 < total3) & (offset3_d + j3 < KEPT)
    policy2 = full(24) * 16 + full(28)
    via = s_f * 1024 + slot2
    stack = jnp.concatenate(
        [
            (jnp.minimum(cum2, float(SLOTS)) - half).astype(BF16),
            (jnp.minimum(ex2, float(SLOTS)) - half).astype(BF16),
            parent1.astype(BF16),
            high1.astype(BF16),
            low1.astype(BF16),
        ],
        axis=0,
    )
    path3, policy3 = [], []
    for r in range(CAP):
        j = j3[r : r + 1]
        hit = (ex3 <= j) & (j < cum3)
        policy3.append(jnp.sum(jnp.where(hit, policy2, 0.0), axis=0, keepdims=True))
        through = jnp.sum(jnp.where(hit, via, 0.0), axis=0, keepdims=True).astype(I32)
        device = lax.shift_right_logical(through, 10)
        jj = (through & 1023).astype(F32) - half
        got = mm(stack, flag(loc0 == device), NN)
        hit = (got[n : 2 * n] <= jj) & (jj < got[:n])
        path = (location * FRONT + got[2 * n : 3 * n]) * POLICY + got[3 * n : 4 * n] * 16 + got[4 * n :]
        path3.append(jnp.sum(jnp.where(hit, path, 0.0), axis=0, keepdims=True))
    path3 = jnp.concatenate(path3, axis=0).astype(I32)
    policy3 = jnp.concatenate(policy3, axis=0).astype(I32)

    def last(ok, base):
        return jnp.where(ok, (mine(base) * 16 + mine(base + 4)).astype(I32), POLICY)

    out_ref[0:4] = floc1.astype(I32)
    out_ref[4:8] = jnp.where(ok1, q1.astype(I32), POLICY)
    out_ref[8:12] = lax.shift_right_logical(path2, 11)
    out_ref[12:16] = path2 & (POLICY - 1)
    out_ref[16:20] = last(ok2, 20)
    out_ref[20:24] = lax.shift_right_logical(path3, 11)
    out_ref[24:28] = path3 & (POLICY - 1)
    out_ref[28:32] = policy3
    out_ref[32:36] = last(ok3, 32)
    out_ref[36:40] = jnp.zeros((4, DEVICES), I32)


FIELDS = ((0, (4,)), (8, (12, 16)), (20, (24, 28, 32)))


def values_kernel(
    core_ref,
    mine_ref,
    other_ref,
    policy_hbm,
    in_hbm,
    out_w_hbm,
    out_hbm,
    table_ref,
    wide_ref,
    found_ref,
    paths_ref,
    ranges_ref,
    front_ref,
    policy_ref,
    in_ref,
    out_w_ref,
    a_ref,
    b_ref,
    c_ref,
    y_ref,
    x0_ref,
    x1_ref,
    h_ref,
    v0_ref,
    v1_ref,
    sems,
):
    def load(src, dst, k):
        copy = pltpu.make_async_copy(src, dst, sems.at[k])
        copy.start()
        return copy

    halves = (mine_ref, other_ref)
    table_loads = [load(ref.at[:, pl.ds(FROWS, TROWS), :], table_ref.at[k], k) for k, ref in enumerate(halves)]
    range_loads = [load(ref.at[:, pl.ds(0, FROWS), :], ranges_ref.at[k], 2 + k) for k, ref in enumerate(halves)]
    policy_load = load(policy_hbm, policy_ref, 4)
    in_load = load(in_hbm, in_ref, 5)
    out_w_load = load(out_w_hbm, out_w_ref, 6)
    for copy in table_loads:
        copy.wait()
    follow(core_ref[0], table_ref, found_ref, wide_ref)
    found_copy = load(found_ref, paths_ref, 7)
    for half in range(2):
        range_loads[half].wait()

        @pl.loop(0, CHIPS // 16)
        def _(j, half=half):
            for e in range(16):
                i = j * 16 + e
                at = (half * CHIPS + i) * (FRONT * CHUNKS)
                for k in range(CHUNKS - 1):
                    wide = ranges_ref[half, i, k * FRONT : (k + 1) * FRONT].astype(F32)
                    front_ref[pl.ds(at + k, FRONT, stride=CHUNKS), :] = wide
                tail = table_ref[half, i, COMMON:].astype(F32)
                front_ref[pl.ds(at + CHUNKS - 1, 8, stride=CHUNKS), :] = tail
                front_ref[pl.ds(at + 9 * CHUNKS - 1, 8, stride=CHUNKS), :] = pltpu.roll(tail, 64, 1)

    found_copy.wait()
    policy_load.wait()

    def rows_of(table, index):
        at = index * CHUNKS
        return table[pl.ds(at, 8), :], table[pl.ds(at + 8, 8), :]

    def rounded(t):
        return t.astype(BF16).astype(F32)

    def chunk(ref, start, k):
        return ref[pl.ds(start * STRIDE + k, 8, stride=STRIDE), :]

    def form(level, first, x_ref):
        place, policies = FIELDS[level]
        hold = (a_ref, b_ref, c_ref)[: level + 1]
        s0 = first // CAP if isinstance(first, int) else lax.shift_right_logical(first, 2)
        for e in range(UNROLL):
            s, r = s0 + e // CAP, e % CAP
            for k, (base, ref) in enumerate(zip(policies, hold)):
                lo, hi = rows_of(policy_ref, paths_ref[base + r, s])
                if k == 0:
                    flo, fhi = rows_of(front_ref, paths_ref[place + r, s])
                    lo, hi = lo * flo, hi * fhi
                ref[e * STRIDE : e * STRIDE + 8, :] = lo
                ref[e * STRIDE + 8 : e * STRIDE + 16, :] = hi
        scales = [None] * (UNROLL // 8)
        for step, ref in enumerate(hold):
            masses = []
            for u in range(UNROLL // 8):
                at = slice(u * 8, u * 8 + 8)
                mass = None
                for k in range(CHUNKS):
                    term = chunk(ref, u * 8, k)
                    cut = slice(k * 128, (k + 1) * 128)
                    if step:
                        term = term * rounded(y_ref[at, cut] * scales[u])
                    y_ref[at, cut] = term
                    mass = term if mass is None else mass + term
                masses.append(mass)
            masses = [jnp.sum(m, axis=1, keepdims=True) for m in masses]
            scales = [jnp.where(m > 0, HANDS / m, 0.0) for m in masses]
        for u in range(UNROLL // 16):
            at = pl.multiple_of(first + u * 16, 16)
            for k in range(CHUNKS):
                cut = slice(k * 128, (k + 1) * 128)
                pair = [y_ref[u * 16 + v * 8 : u * 16 + v * 8 + 8, cut] * scales[2 * u + v] for v in range(2)]
                x_ref[pl.ds(at, 16), cut] = jnp.concatenate(pair, axis=0).astype(BF16)

    for i in range(SLOTS // UNROLL):
        form(0, i * UNROLL, x0_ref)

    xs, vs, stores = (x0_ref, x1_ref), (v0_ref, v1_ref), [None, None]
    in_load.wait()
    out_w_load.wait()
    for level in range(3):
        x_ref, v_ref, ahead = xs[level % 2], vs[level % 2], xs[(level + 1) % 2]
        if stores[level % 2] is not None:
            stores[level % 2].wait()

        for i in range(3):
            if level < 2:
                form(level + 1, i * UNROLL, ahead)
            cut = slice(i * 512, i * 512 + 512)
            hidden = jnp.dot(x_ref[...], in_ref[:, cut], preferred_element_type=F32)
            h_ref[:, cut] = jnp.maximum(hidden, 0.0).astype(BF16)

        def second(cut, v_ref=v_ref):
            value = lax.dot_general(out_w_ref[cut, :], h_ref[...], (NT, ((), ())), preferred_element_type=F32)
            v_ref[cut, :] = value.astype(BF16)

        for i in range(5):
            if level < 2:
                form(level + 1, (i + 3) * UNROLL, ahead)
            second(slice(i * 256, i * 256 + 256))

        second(slice(1280, HANDS))
        stores[level % 2] = load(v_ref, out_hbm.at[level], 8 + level % 2)
    for copy in stores:
        copy.wait()


def values(core, mine, other, policy, value_in, value_out):
    hbm = pl.BlockSpec(memory_space=pl.ANY)
    hold = pltpu.VMEM((UNROLL * STRIDE + 16, 128), F32)
    return pl.pallas_call(
        values_kernel,
        out_shape=jax.ShapeDtypeStruct((3, HANDS, SLOTS), BF16),
        in_specs=[pl.BlockSpec(memory_space=pltpu.SMEM), hbm, hbm, hbm, hbm, hbm],
        out_specs=hbm,
        scratch_shapes=[
            pltpu.VMEM((2, CHIPS, TROWS, 128), BF16),
            pltpu.VMEM((2, CHIPS * TROWS, 128), F32),
            pltpu.VMEM((40, 128), I32),
            pltpu.SMEM((40, 128), I32),
            pltpu.VMEM((2, CHIPS, FROWS, 128), BF16),
            pltpu.VMEM((DEVICES * FRONT * CHUNKS + 8, 128), F32),
            pltpu.VMEM(policy.shape, F32),
            pltpu.VMEM((WIDTH, HIDDEN), BF16),
            pltpu.VMEM((HANDS, HIDDEN), BF16),
            hold,
            hold,
            hold,
            pltpu.VMEM((UNROLL, WIDTH), F32),
            pltpu.VMEM((SLOTS, WIDTH), BF16),
            pltpu.VMEM((SLOTS, WIDTH), BF16),
            pltpu.VMEM((SLOTS, HIDDEN), BF16),
            pltpu.VMEM((HANDS, SLOTS), BF16),
            pltpu.VMEM((HANDS, SLOTS), BF16),
            pltpu.SemaphoreType.DMA((10,)),
        ],
        compiler_params=pltpu.CompilerParams(vmem_limit_bytes=62 * 1024 * 1024),
        name="values",
    )(core, mine, other, policy, value_in, value_out)


def on_device(frontier, policy_table, first, policy_index, owner_index, following, value_in, value_out):
    core = lax.axis_index("owner_3").astype(I32)[None]
    block = tables(first, owner_index, policy_index, following, frontier)
    mine = lax.all_to_all(block, OWNER[:3], split_axis=0, concat_axis=0, tiled=True)
    policy = jnp.pad(policy_table, ((0, 1), (0, WIDTH - HANDS))).astype(F32).reshape((POLICY + 1) * CHUNKS, 128)
    policy = jnp.pad(policy, ((0, 13), (0, 0)))
    weights_in = jnp.pad(value_in, ((0, WIDTH - HANDS), (0, 0)))
    mine, policy, weights_in = lax.optimization_barrier((mine, policy, weights_in))
    other = lax.ppermute(mine, OWNER[3], [(0, 1), (1, 0)])

    out = values(core, mine, other, policy, weights_in, jnp.transpose(value_out))
    return jnp.transpose(out, (0, 2, 1))


def solution(mesh):
    torus = Mesh(mesh.devices.reshape(4, 4, 4, 2), OWNER)
    placed = (P(OWNER, None), P(), P(OWNER), P(None, OWNER), P(None, OWNER), P(None, OWNER), P(), P())
    return jax.shard_map(on_device, mesh=torus, in_specs=placed, out_specs=P(None, OWNER, None), check_vma=False)
```
